32 devices in a mesh: ga: 8 (over z, x), band: 4 (over y, core).
Axes of the slice: x: 2, y: 2, z: 4, core: 2. Of those that a mesh axis runs over, the one named last changes fastest.
Arguments:
- waves: float32 [2, 8192, 1024], P(None, 'ga', 'band'), may hold values from -6 to 6
- miller: int32 [3, 8192], P(None, 'ga'), may hold values from -8 to 8
- positions: float32 [64, 3], replicated, may hold values from 0 to 1
- form_factors: float32 [4, 18, 8192], P(None, None, 'ga'), may hold values from -0.0625 to 0.0625
- coupling: float32 [4, 18, 18], replicated, may hold values from -1.6970563 to 5.656854
- species: int32 [64], replicated, may hold values from 0 to 3
- block_sizes: int32 [64], replicated, may hold values from 1 to 18, 512 in all
- occupation: float32 [1024], P('band'), may hold values from 0.05 to 2
Outputs:
- residual: float32 [2, 8192, 1024], P(None, 'ga', 'band')
- estimate: float32 [1024], P('band')
- energy: float32 [], replicated
The draws below stay inside these ranges and needn't reach their ends.
All inputs are finite; a program needn't handle non-finite values.
Results may differ from the reference program's by a relative error of at most 0.00007.
Values sent between devices are 32-bit elements; how exact they have to be, the bound alone decides.
No kernel may reach another device: no remote copies, remote signals or barrier semaphores. Data moves between devices by JAX's collectives and lax.ppermute only.
A program may use at most 64 MiB of HBM per device.

```python
import math
import jax
import jax.numpy as jnp
import numpy as np
from jax import lax

ATOMS = 64
KMAX = 18
NSPEC = 4
PROJ = 512
NG = 8192
NB = 1024


def draw_coupling(key, part):
    scale = (NG / (8.0 * PROJ)) ** 0.5
    first_key, second_key = jax.random.split(jax.random.fold_in(key, 11))
    offdiag = jnp.clip(0.3 * jax.random.normal(first_key, (NSPEC, KMAX, KMAX), jnp.float32), -1.2, 1.2)
    diagonal = jnp.exp(jax.random.uniform(second_key, (NSPEC, KMAX), jnp.float32, 0.0, math.log(4.0)))
    identity = jnp.eye(KMAX, dtype=jnp.float32)
    return scale * (offdiag * (1.0 - identity) + diagonal[:, :, None] * identity)


def plant(result, rng, least, top_value):
    dims = result.shape
    index_at = [jax.random.randint(jax.random.fold_in(rng, axis), (), 0, dims[axis]) for axis in range(len(dims))]
    result = result.at[tuple(index_at)].set(least)
    longest = dims.index(max(dims))
    index_at[longest] = (index_at[longest] + 1) % dims[longest]
    return result.at[tuple(index_at)].set(top_value)


def raised(result, own_key, source, target, parts, factor):
    owner, partner = [(jnp.arange(result.shape[position]) // (result.shape[position] // parts)).reshape([-1 if axis == position else 1 for axis in range(result.ndim)]) for position in (source, target)]
    chosen = jax.random.permutation(own_key, parts)[partner]
    strong = (owner == chosen) | (owner == (partner + parts // 2) % parts)
    return jnp.where(strong, factor * result, result)


def shard_levels(key, extent, cuts, low, top_value):
    def one(dim, shards_of):
        draws = jax.random.uniform(jax.random.fold_in(jax.random.fold_in(key, 6), dim), (shards_of,), jnp.float32, low / len(cuts), top_value / len(cuts))
        return jnp.repeat(jnp.exp(draws), extent[dim] // shards_of).reshape((-1,) + (1,) * (len(extent) - dim - 1))

    level = one(*cuts[0])
    for cut in cuts[1:]:
        level = level * one(*cut)
    return level


def profile(amount, total, bound, lean):
    portions = [(1 << 20) // math.isqrt(grade ** lean) + 1 for grade in range(2, amount + 1)]
    rest, holding = total - bound - (amount - 1), [1] * (amount - 1)
    while rest > 0:
        movable = [i for i in range(amount - 1) if holding[i] < bound]
        mass, left = sum([portions[i] for i in movable]), rest
        for i in movable:
            extra = min(bound - holding[i], max(1, left * portions[i] // mass), rest)
            holding[i] = holding[i] + extra
            rest = rest - extra
    return np.array([bound] + holding)


def uneven_parts(stream_key, amount, total, bound, skew):
    if amount == 2:
        one = jax.random.randint(stream_key, (), max(1, total - bound), min(bound, total - 1) + 1)
        return jnp.stack([one, total - one])
    tallies = jnp.asarray(profile(amount, total, bound, skew), jnp.int32)
    pairs = (amount - 1) // 2
    giver, receiver = tallies[1:1 + 2 * pairs:2], tallies[2:2 + 2 * pairs:2]
    slack = jnp.minimum(giver - 1, bound - receiver)
    moved = jax.random.randint(jax.random.fold_in(stream_key, 1), (pairs,), 0, 1 << 20) % (slack + 1)
    tallies = tallies.at[1:1 + 2 * pairs:2].set(giver - moved).at[2:2 + 2 * pairs:2].set(receiver + moved)
    return tallies[jax.random.permutation(jax.random.fold_in(stream_key, 2), amount)]


def scatter_about(rng, shape, spread, reach, cuts=(), kind=jnp.bfloat16):
    entries = spread * jax.random.normal(rng, shape, jnp.float32)
    if cuts:
        entries = entries * shard_levels(rng, shape, cuts, -0.22, 0.18)
    return jnp.clip(entries, -reach, reach).astype(kind)


def heavy_noise(own_key, dims, deviation, reach, cuts, heavy, kind=jnp.bfloat16):
    array = deviation * jax.random.normal(own_key, dims, jnp.float32)
    if cuts:
        array = array * shard_levels(own_key, dims, cuts, -0.22, 0.18)
    return jnp.clip(raised(array, jax.random.fold_in(own_key, 3), *heavy), -reach, reach).astype(kind)


def setup_inputs(seed: int = 0) -> dict:
    streams_of = jax.random.split(jax.random.key(seed), 9)
    waves = heavy_noise(streams_of[0], (2, NG, NB), 1.0, 6.0, ((1, 8), (2, 4)), (1, 2, 8, 2.0), jnp.float32)
    miller = plant(jax.random.randint(streams_of[1], (3, NG), -8, 9), jax.random.fold_in(streams_of[1], 1), -8, 8).astype(jnp.int32)
    positions = jnp.clip(jax.random.uniform(streams_of[2], (ATOMS, 3), jnp.float32, 0.0, 1.0), 0.0, 1.0)
    form_factors = scatter_about(streams_of[3], (NSPEC, KMAX, NG), NG ** -0.5, 0.0625, ((2, 8),), jnp.float32)
    coupling = draw_coupling(jax.random.fold_in(streams_of[8], 71), 0)
    species = plant(jax.random.randint(streams_of[5], (ATOMS,), 0, NSPEC), jax.random.fold_in(streams_of[5], 1), 0, NSPEC - 1).astype(jnp.int32)
    block_sizes = uneven_parts(streams_of[6], ATOMS, PROJ, KMAX, 1).astype(jnp.int32)
    occupation = jnp.clip(jnp.exp(math.log(2.0) - 3.6888794 * jax.random.uniform(streams_of[7], (NB,), jnp.float32) ** shard_levels(streams_of[7], (NB,), ((0, 4),), -0.2, 0.2)), 0.05, 2.0)
    return dict(waves=waves, miller=miller, positions=positions, form_factors=form_factors, coupling=coupling, species=species, block_sizes=block_sizes, occupation=occupation)


TWO_PI = 6.283185307179586
KINETIC_SCALE = 0.005
EPSILON = 1e-6
HIGHEST_PRECISION = lax.Precision.HIGHEST


def reference(waves, miller, positions, form_factors, coupling, species, block_sizes, occupation):
    block_ends = jnp.cumsum(block_sizes).astype(jnp.int32)
    block_starts = (block_ends - block_sizes).astype(jnp.int32)
    columns = jnp.arange(PROJ, dtype=jnp.int32)
    owner_atom = jnp.sum((block_ends[None, :] <= columns[:, None]).astype(jnp.int32), axis=1).astype(jnp.int32)
    channel = (columns - jnp.take(block_starts, owner_atom)).astype(jnp.int32)
    row_index = (jnp.take(species, owner_atom) * KMAX + channel).astype(jnp.int32)
    radial = jnp.take(form_factors.reshape(NSPEC * KMAX, NG), row_index, axis=0)
    miller_f = miller.astype(jnp.float32)
    phases = TWO_PI * (positions[:, 0:1] * miller_f[0][None, :] + positions[:, 1:2] * miller_f[1][None, :] + positions[:, 2:3] * miller_f[2][None, :])
    beta_re = radial * jnp.take(jnp.cos(phases), owner_atom, axis=0)
    beta_im = -(radial * jnp.take(jnp.sin(phases), owner_atom, axis=0))
    table = jnp.take(coupling.reshape(NSPEC * KMAX, KMAX), row_index, axis=0)
    dense = jnp.take(table, channel, axis=1)
    dense = jnp.where(owner_atom[:, None] == owner_atom[None, :], dense, jnp.zeros_like(dense))
    psi_re = waves[0]
    psi_im = waves[1]
    proj_re = jnp.dot(beta_re, psi_re, precision=HIGHEST_PRECISION) + jnp.dot(beta_im, psi_im, precision=HIGHEST_PRECISION)
    proj_im = jnp.dot(beta_re, psi_im, precision=HIGHEST_PRECISION) - jnp.dot(beta_im, psi_re, precision=HIGHEST_PRECISION)
    kinetic = 0.5 * KINETIC_SCALE * (miller_f[0] * miller_f[0] + miller_f[1] * miller_f[1] + miller_f[2] * miller_f[2])
    density = psi_re * psi_re + psi_im * psi_im
    kin_sum = jnp.sum(kinetic[:, None] * density, axis=0)
    norm_sum = jnp.sum(density, axis=0)
    mixed_re = jnp.dot(dense, proj_re, precision=HIGHEST_PRECISION)
    mixed_im = jnp.dot(dense, proj_im, precision=HIGHEST_PRECISION)
    nonlocal_sum = jnp.sum(proj_re * mixed_re + proj_im * mixed_im, axis=0)
    estimate = (kin_sum + nonlocal_sum) / (norm_sum + EPSILON)
    contract = (((0,), (0,)), ((), ()))
    applied_re = lax.dot_general(beta_re, mixed_re, contract, precision=HIGHEST_PRECISION) - lax.dot_general(beta_im, mixed_im, contract, precision=HIGHEST_PRECISION)
    applied_im = lax.dot_general(beta_re, mixed_im, contract, precision=HIGHEST_PRECISION) + lax.dot_general(beta_im, mixed_re, contract, precision=HIGHEST_PRECISION)
    shifted = kinetic[:, None] - estimate[None, :]
    residual = jnp.stack([shifted * psi_re + applied_re, shifted * psi_im + applied_im])
    energy = jnp.sum(occupation * nonlocal_sum / (norm_sum + EPSILON))
    return residual, estimate, energy
```

```python
import functools
import math

import jax
import jax.numpy as jnp
from jax import lax
from jax.experimental import pallas as pl
from jax.experimental.pallas import tpu as pltpu
from jax.sharding import PartitionSpec as P

PROJ = 512
KINETIC_SCALE = 0.005
EPSILON = 1e-06
LANES = 128
F32 = jnp.float32
BF16 = jnp.bfloat16


def iota(shape, dim):
    return lax.broadcasted_iota(jnp.int32, shape, dim)


def split(x):
    hi = x.astype(BF16)
    return hi, (x - hi.astype(F32)).astype(BF16)


def dot(a, b, contract=((1,), (0,))):
    return lax.dot_general(a, b, (contract, ((), ())), preferred_element_type=F32)


def pick(mask, values, axis):
    return jnp.sum(jnp.where(mask, values, 0.0), axis=axis, keepdims=True)


def stride_of(kmax):
    return -(-kmax // 16) * 16


def columns_of(sizes, species):
    atoms = sizes.shape[1]
    here, there = iota((atoms, atoms), 0), iota((atoms, atoms), 1)
    start = pick(there < here, sizes, 1)
    size = pick(there == here, sizes, 1)
    spec = pick(there == here, species, 1)
    return start, size, spec


def rows_by_projector(sizes, species, stride):
    atoms = sizes.shape[1]
    _, size, spec = columns_of(sizes, species)
    atom = lax.rem(iota((atoms, 2 * atoms), 1), atoms)
    here = iota((atoms, 2 * atoms), 0)
    start = pick(here < atom, size, 0)
    end = start + pick(here == atom, size, 0)
    spec = pick(here == atom, spec, 0)
    column = iota((PROJ, 2 * atoms), 0).astype(F32)
    hot = (column >= start) & (column < end)
    lane = iota((PROJ, 2 * atoms), 1)
    first = hot & (lane < atoms)
    row = pick(first, stride * spec - start, 1) + iota((PROJ, 1), 0).astype(F32)
    owner = pick(first, lane.astype(F32), 1)
    return row, jnp.where(hot, 1.0, 0.0).astype(BF16), owner


def rows_by_lane(sizes, species, stride):
    atoms = sizes.shape[1]
    start, size, spec = columns_of(sizes, species)
    column = iota((atoms, PROJ), 1).astype(F32)
    hot = (column >= start) & (column < start + size)
    lane = iota((1, PROJ), 1).astype(F32)
    channel = lane - pick(hot, start, 0)
    row = channel + pick(hot, stride * spec, 0)
    owner = pick(hot, iota((atoms, PROJ), 0).astype(F32), 0)
    ones = jnp.where(hot, 1.0, 0.0)
    return row, jnp.concatenate([ones, ones], axis=0).astype(BF16), owner, channel


def trig(positions, miller):
    cycles = (
        positions[:, 0:1] * miller[0:1] + positions[:, 1:2] * miller[1:2] + positions[:, 2:3] * miller[2:3]
    )
    half = (cycles - jnp.round(cycles)) * math.pi
    sq = half * half
    sine = 1.0 / 6227020800.0
    for n in (39916800.0, 362880.0, 5040.0, 120.0, 6.0, 1.0):
        sine = 1.0 / n - sq * sine
    sine = half * sine
    cosine = 1.0 / 479001600.0
    for n in (3628800.0, 40320.0, 720.0, 24.0, 2.0, 1.0):
        cosine = 1.0 / n - sq * cosine
    return 1.0 - 2.0 * sine * sine, 2.0 * sine * cosine


def stacked(x):
    hi, lo = split(x)
    return jnp.concatenate([hi, lo], axis=0)


def fill_rows(scratch, table, stride):
    nspec, kmax, width = table.shape
    scratch[...] = jnp.zeros(scratch.shape, F32)
    for s in range(nspec):
        scratch[s * stride : s * stride + kmax, 0:width] = table[s]


def hot_rows(row, depth):
    j = lax.rem(iota((PROJ, 2 * depth), 1), depth).astype(F32)
    return jnp.where(row == j, 1.0, 0.0).astype(BF16)


def hot_rows_t(row, depth):
    j = lax.rem(iota((2 * depth, PROJ), 0), depth).astype(F32)
    return jnp.where(row == j, 1.0, 0.0).astype(BF16)


def squares(miller):
    total = miller[0:1] * miller[0:1] + miller[1:2] * miller[1:2] + miller[2:3] * miller[2:3]
    return total


def bit(device, b):
    return lax.rem(lax.shift_right_logical(device, b), 2)


def block_row(device, order, rel, rows):
    index = 2 * lax.bitwise_xor(bit(device, order[0]), rel[0]) + lax.bitwise_xor(bit(device, order[1]), rel[1])
    return pl.multiple_of(index * rows, rows)


def project_kernel(orders, waves, miller, positions, form, species, sizes, *refs):
    outs, (table, hi_ref, lo_ref, rhs_hi, rhs_lo, full) = refs[:4], refs[4:]
    planes = miller.shape[1]
    half = waves.shape[2] // 2
    rows = PROJ // 4
    device = lax.axis_index("ga")
    stride = stride_of(form.shape[1])
    depth = stride * form.shape[0]
    fill_rows(table, form, stride)
    m = miller[...].astype(F32)
    cosine, sine = trig(positions[...], m)
    cosine, sine = stacked(cosine), stacked(sine)
    radial = stacked(table[...])
    row, owners, _ = rows_by_projector(sizes[...].astype(F32), species[...].astype(F32), stride)
    picks = hot_rows(row, depth)
    for r in range(4):
        part = slice(r * rows, (r + 1) * rows)
        size = dot(picks[part], radial)
        hi, lo = split(size * dot(owners[part], cosine))
        hi_ref[part, 0:planes] = hi
        lo_ref[part, 0:planes] = lo
        hi, lo = split(-(size * dot(owners[part], sine)))
        hi_ref[part, planes : 2 * planes] = hi
        lo_ref[part, planes : 2 * planes] = lo
    weight = jnp.where(iota((8, planes), 0) == 0, squares(m), 1.0).astype(BF16)
    scale = jnp.where(iota((8, half), 0) == 0, 0.5 * KINETIC_SCALE, 1.0)
    for q, order in enumerate(orders):
        bands = slice(q * half, (q + 1) * half)
        re, im = waves[0, :, bands], waves[1, :, bands]
        dens_hi, dens_lo = split(re * re + im * im)
        sums = scale * (dot(weight, dens_hi) + dot(weight, dens_lo))
        re_hi, re_lo = split(re)
        im_hi, im_lo = split(im)
        for ref, a, b in ((rhs_hi, re_hi, im_hi), (rhs_lo, re_lo, im_lo)):
            ref[0:planes, 0:half] = a
            ref[0:planes, half:] = b
            ref[planes:, 0:half] = b
            ref[planes:, half:] = -a
        full[...] = (
            dot(hi_ref[...], rhs_hi[...]) + dot(hi_ref[...], rhs_lo[...]) + dot(lo_ref[...], rhs_hi[...])
        )
        tail = jnp.concatenate([sums, jnp.zeros_like(sums)], axis=1)
        for first, out in ((1, outs[2 * q]), (0, outs[2 * q + 1])):
            for second in (0, 1):
                at = block_row(device, order, (first, second), rows)
                out[second * rows : (second + 1) * rows] = full[pl.ds(at, rows)]
            out[2 * rows :] = tail


def apply_tables_kernel(miller, positions, form, coupling, species, sizes, hi_ref, lo_ref, dense_hi, dense_lo, table, ctable):
    planes = miller.shape[1]
    stride = stride_of(form.shape[1])
    depth = stride * form.shape[0]
    fill_rows(table, form, stride)
    fill_rows(ctable, coupling, stride)
    m = miller[...].astype(F32)
    cosine, sine = trig(positions[...], m)
    cosine, sine = stacked(cosine), stacked(sine)
    radial = stacked(table[...])
    lengths, kinds = sizes[...].astype(F32), species[...].astype(F32)
    row, owners, owner_row, channel = rows_by_lane(lengths, kinds, stride)
    picks = hot_rows_t(row, depth)
    step = planes // 4
    over = ((0,), (0,))
    for r in range(4):
        part = slice(r * step, (r + 1) * step)
        size = dot(radial[:, part], picks, over)
        hi, lo = split(size * dot(cosine[:, part], owners, over))
        hi_ref[part, 0:PROJ] = hi
        lo_ref[part, 0:PROJ] = lo
        hi, lo = split(-(size * dot(sine[:, part], owners, over)))
        hi_ref[part, PROJ : 2 * PROJ] = hi
        lo_ref[part, PROJ : 2 * PROJ] = lo
    row, _, owner_col = rows_by_projector(lengths, kinds, stride)
    lines = dot(hot_rows(row, depth), stacked(ctable[...]))
    lines_hi, lines_lo = split(lines)
    spread = jnp.where(iota((ctable.shape[1], PROJ), 0).astype(F32) == channel, 1.0, 0.0).astype(BF16)
    dense = dot(lines_hi, spread) + dot(lines_lo, spread)
    hi, lo = split(jnp.where(owner_col == owner_row, dense, 0.0))
    dense_hi[...] = hi
    dense_lo[...] = lo


def finish_kernel(order, own, near, far, sums, waves, miller, occupation, hi_ref, lo_ref, dense_hi, dense_lo, *refs):
    residual, estimate, share, full, rhs_hi, rhs_lo = refs[-6:]
    rows = PROJ // 4
    half = occupation.shape[1]
    device = lax.axis_index("ga")
    for rel, ref, at in (((0, 0), own, 0), ((0, 1), near, 0), ((1, 0), far, 0), ((1, 1), far, rows)):
        full[pl.ds(block_row(device, order, rel, rows), rows)] = ref[at : at + rows]
    proj = full[...]
    p_hi, p_lo = split(proj)
    mixed = dot(dense_hi[...], p_hi) + dot(dense_hi[...], p_lo) + dot(dense_lo[...], p_hi)
    pairs = jnp.sum(proj * mixed, axis=0, keepdims=True)
    nonlocal_sum = pairs[:, 0:half] + pairs[:, half:]
    kin, norm = sums[0:1, 0:half], sums[1:2, 0:half]
    level = (kin + nonlocal_sum) / (norm + EPSILON)
    estimate[...] = level
    share[...] = occupation[...] * (nonlocal_sum / (norm + EPSILON))
    m_hi, m_lo = split(mixed)
    for ref, m in ((rhs_hi, m_hi), (rhs_lo, m_lo)):
        ref[0:PROJ] = m
        ref[PROJ:, 0:half] = -m[:, half:]
        ref[PROJ:, half:] = m[:, 0:half]
    planes = miller.shape[1]
    step = planes // 4
    unit = jnp.where(iota((8, half), 0) == 0, 1.0, 0.0).astype(BF16)
    for r in range(4):
        part = slice(r * step, (r + 1) * step)
        applied = dot(hi_ref[part], rhs_hi[...]) + dot(hi_ref[part], rhs_lo[...]) + dot(lo_ref[part], rhs_hi[...])
        m = miller[:, part].astype(F32)
        line = jnp.broadcast_to(squares(m), (8, step)).astype(BF16)
        kinetic = (0.5 * KINETIC_SCALE) * dot(line, unit, ((0,), (0,)))
        shifted = kinetic - level
        residual[0, part] = shifted * waves[0, part] + applied[:, 0:half]
        residual[1, part] = shifted * waves[1, part] + applied[:, half:]


def whole(shape):
    return pl.BlockSpec(shape, lambda *_: (0,) * len(shape))


def swap(x, axis, size, b):
    return lax.ppermute(x, axis, [(i, i ^ (1 << b)) for i in range(size)])


def on_device(ga, band, waves, miller, positions, form_factors, coupling, species, block_sizes, occupation):
    _, planes, bands = waves.shape
    half = bands // 2
    nspec, kmax, _ = form_factors.shape
    rows = PROJ // 4
    depth = stride_of(kmax) * nspec
    species = species.reshape(1, -1)
    sizes = block_sizes.reshape(1, -1)
    bits = ga.bit_length() - 1
    orders = ((0, 1), (1, 0))
    outs = pl.pallas_call(
        functools.partial(project_kernel, orders),
        name="project",
        out_shape=[jax.ShapeDtypeStruct((2 * rows + 8, bands), F32)] * 4,
        scratch_shapes=[
            pltpu.VMEM((depth, planes), F32),
            pltpu.VMEM((PROJ, 2 * planes), BF16),
            pltpu.VMEM((PROJ, 2 * planes), BF16),
            pltpu.VMEM((2 * planes, bands), BF16),
            pltpu.VMEM((2 * planes, bands), BF16),
            pltpu.VMEM((PROJ, bands), F32),
        ],
        compiler_params=pltpu.CompilerParams(vmem_limit_bytes=48 * 1024 * 1024),
    )(waves, miller, positions, form_factors, species, sizes)
    tables = pl.pallas_call(
        apply_tables_kernel,
        name="apply_tables",
        out_shape=[jax.ShapeDtypeStruct((planes, 2 * PROJ), BF16)] * 2 + [jax.ShapeDtypeStruct((PROJ, PROJ), BF16)] * 2,
        scratch_shapes=[pltpu.VMEM((depth, planes), F32), pltpu.VMEM((depth, LANES), F32)],
        compiler_params=pltpu.CompilerParams(vmem_limit_bytes=48 * 1024 * 1024),
    )(miller, positions, form_factors, coupling, species, sizes)
    got = [swap(outs[2 * q], "ga", ga, order[0]) for q, order in enumerate(orders)]
    kept = [outs[2 * q + 1] + got[q] for q in range(2)]
    got = [swap(kept[q][rows:], "ga", ga, order[1]) for q, order in enumerate(orders)]
    mine = [
        jnp.concatenate([kept[q][:rows] + got[q][:rows], kept[q][2 * rows :] + got[q][rows:]], axis=0)
        for q in range(2)
    ]
    for b in range(2, bits):
        got = [swap(mine[q], "ga", ga, b) for q in range(2)]
        mine = [mine[q] + got[q] for q in range(2)]
    own = [mine[q][:rows] for q in range(2)]
    near = [swap(own[q], "ga", ga, order[1]) for q, order in enumerate(orders)]
    far = [swap(jnp.concatenate([own[q], near[q]], axis=0), "ga", ga, order[0]) for q, order in enumerate(orders)]
    residual = None
    levels, shares = [], []
    occ = occupation.reshape(2, half)
    for q, order in enumerate(orders):
        operands = [own[q], near[q], far[q], mine[q][rows:], waves, miller, occ[q : q + 1], *tables]
        specs = [whole(x.shape) for x in operands]
        specs[4] = pl.BlockSpec((2, planes, half), lambda i, q=q: (0, 0, q))
        alias = {}
        if residual is not None:
            alias = {len(operands): 0}
            operands.append(residual)
            specs.append(pl.BlockSpec(memory_space=pl.ANY))
        residual, level, share = pl.pallas_call(
            functools.partial(finish_kernel, order),
            name=f"finish{q}",
            grid=(1,),
            in_specs=specs,
            out_specs=[
                pl.BlockSpec((2, planes, half), lambda i, q=q: (0, 0, q)),
                whole((1, half)),
                whole((1, half)),
            ],
            out_shape=[
                jax.ShapeDtypeStruct(waves.shape, F32),
                jax.ShapeDtypeStruct((1, half), F32),
                jax.ShapeDtypeStruct((1, half), F32),
            ],
            scratch_shapes=[
                pltpu.VMEM((PROJ, bands), F32),
                pltpu.VMEM((2 * PROJ, bands), BF16),
                pltpu.VMEM((2 * PROJ, bands), BF16),
            ],
            input_output_aliases=alias,
            compiler_params=pltpu.CompilerParams(vmem_limit_bytes=48 * 1024 * 1024),
        )(*operands)
        levels.append(level)
        shares.append(share)
    energy = jnp.sum(shares[0] + shares[1]).reshape(1, 1)
    for b in range(band.bit_length() - 1):
        energy = energy + swap(energy, "band", band, b)
    estimate = jnp.concatenate(levels, axis=0).reshape(bands)
    return residual, estimate, energy.reshape(())


def solution(mesh):
    in_specs = (
        P(None, "ga", "band"),
        P(None, "ga"),
        P(),
        P(None, None, "ga"),
        P(),
        P(),
        P(),
        P("band"),
    )
    out_specs = (P(None, "ga", "band"), P("band"), P())
    body = functools.partial(on_device, mesh.shape["ga"], mesh.shape["band"])
    return jax.shard_map(body, mesh=mesh, in_specs=in_specs, out_specs=out_specs, check_vma=False)
```

```python
import functools
import math

import jax
import jax.numpy as jnp
from jax import lax
from jax.experimental import pallas as pl
from jax.experimental.pallas import tpu as pltpu
from jax.sharding import PartitionSpec as P

PROJ = 512
KINETIC_SCALE = 0.005
EPSILON = 1e-06
LANES = 128
F32 = jnp.float32
BF16 = jnp.bfloat16


def iota(shape, dim):
    return lax.broadcasted_iota(jnp.int32, shape, dim)


def split(x):
    hi = x.astype(BF16)
    return hi, (x - hi.astype(F32)).astype(BF16)


def dot(a, b, contract=((1,), (0,))):
    return lax.dot_general(a, b, (contract, ((), ())), preferred_element_type=F32)


def pick(mask, values, axis):
    return jnp.sum(jnp.where(mask, values, 0.0), axis=axis, keepdims=True)


def depth_of(kmax, nspec):
    return -(-kmax * nspec // 16) * 16


def columns_of(sizes, species):
    atoms = sizes.shape[1]
    here, there = iota((atoms, atoms), 0), iota((atoms, atoms), 1)
    start = pick(there < here, sizes, 1)
    size = pick(there == here, sizes, 1)
    spec = pick(there == here, species, 1)
    return start, size, spec


def rows_by_projector(sizes, species, nspec):
    atoms = sizes.shape[1]
    _, size, spec = columns_of(sizes, species)
    atom = lax.rem(iota((atoms, 2 * atoms), 1), atoms)
    here = iota((atoms, 2 * atoms), 0)
    start = pick(here < atom, size, 0)
    end = start + pick(here == atom, size, 0)
    spec = pick(here == atom, spec, 0)
    place = iota((PROJ, 2 * atoms), 0).astype(F32)
    hot = (place >= start) & (place < end)
    lane = iota((PROJ, 2 * atoms), 1)
    first = hot & (lane < atoms)
    row = pick(first, spec - nspec * start, 1) + nspec * iota((PROJ, 1), 0).astype(F32)
    owner = pick(first, lane.astype(F32), 1)
    return row, jnp.where(hot, 1.0, 0.0).astype(BF16), owner


def rows_by_lane(sizes, species, nspec):
    atoms = sizes.shape[1]
    start, size, spec = columns_of(sizes, species)
    place = iota((atoms, PROJ), 1).astype(F32)
    hot = (place >= start) & (place < start + size)
    lane = iota((1, PROJ), 1).astype(F32)
    channel = lane - pick(hot, start, 0)
    row = nspec * channel + pick(hot, spec, 0)
    owner = pick(hot, iota((atoms, PROJ), 0).astype(F32), 0)
    ones = jnp.where(hot, 1.0, 0.0)
    return row, jnp.concatenate([ones, ones], axis=0).astype(BF16), owner, channel


def column(rows, n):
    size = rows.shape[1]
    return pick(iota((size, size), 0) == iota((size, size), 1), rows[n : n + 1], 1)


def trig(positions, miller):
    cycles = (
        column(positions, 0) * miller[0:1] + column(positions, 1) * miller[1:2] + column(positions, 2) * miller[2:3]
    )
    half = (cycles - jnp.round(cycles)) * math.pi
    sq = half * half
    sine = 1.0 / 6227020800.0
    for n in (39916800.0, 362880.0, 5040.0, 120.0, 6.0, 1.0):
        sine = 1.0 / n - sq * sine
    sine = half * sine
    cosine = 1.0 / 479001600.0
    for n in (3628800.0, 40320.0, 720.0, 24.0, 2.0, 1.0):
        cosine = 1.0 / n - sq * cosine
    return 1.0 - 2.0 * sine * sine, 2.0 * sine * cosine


def stacked(x):
    hi, lo = split(x)
    return jnp.concatenate([hi, lo], axis=0)


def fill_rows(scratch, table):
    kmax, nspec, width = table.shape
    scratch[...] = jnp.zeros(scratch.shape, F32)
    for k in range(kmax):
        scratch[k * nspec : (k + 1) * nspec, 0:width] = table[k]


def hot_rows(row, depth):
    j = lax.rem(iota((PROJ, 2 * depth), 1), depth).astype(F32)
    return jnp.where(row == j, 1.0, 0.0).astype(BF16)


def hot_rows_t(row, depth):
    j = lax.rem(iota((2 * depth, PROJ), 0), depth).astype(F32)
    return jnp.where(row == j, 1.0, 0.0).astype(BF16)


def squares(miller):
    total = miller[0:1] * miller[0:1] + miller[1:2] * miller[1:2] + miller[2:3] * miller[2:3]
    return total


def bit(device, b):
    return lax.rem(lax.shift_right_logical(device, b), 2)


def block_row(device, order, rel, rows):
    index = 2 * lax.bitwise_xor(bit(device, order[0]), rel[0]) + lax.bitwise_xor(bit(device, order[1]), rel[1])
    return pl.multiple_of(index * rows, rows)


def project_half(order, re, im, miller, hi_ref, lo_ref, outs, rhs_hi, rhs_lo, full):
    planes, half = re.shape
    rows = PROJ // 4
    device = lax.axis_index("ga")
    weight = jnp.where(iota((8, planes), 0) == 0, squares(miller), 1.0).astype(BF16)
    scale = jnp.where(iota((8, half), 0) == 0, 0.5 * KINETIC_SCALE, 1.0)
    dens_hi, dens_lo = split(re * re + im * im)
    sums = scale * (dot(weight, dens_hi) + dot(weight, dens_lo))
    re_hi, re_lo = split(re)
    im_hi, im_lo = split(im)
    for ref, a, b in ((rhs_hi, re_hi, im_hi), (rhs_lo, re_lo, im_lo)):
        ref[0:planes, 0:half] = a
        ref[0:planes, half:] = b
        ref[planes:, 0:half] = b
        ref[planes:, half:] = -a
    full[...] = dot(hi_ref[...], rhs_hi[...]) + dot(hi_ref[...], rhs_lo[...]) + dot(lo_ref[...], rhs_hi[...])
    tail = jnp.concatenate([sums, jnp.zeros_like(sums)], axis=1)
    for first, out in ((1, outs[0]), (0, outs[1])):
        for second in (0, 1):
            out[second * rows : (second + 1) * rows] = full[pl.ds(block_row(device, order, (first, second), rows), rows)]
        out[2 * rows :] = tail


def project_first(order, waves_in, miller_in, positions_in, form_in, species_in, sizes_in, *refs):
    outs, (hi_ref, lo_ref) = refs[:2], refs[2:4]
    waves, miller, positions, form, species, sizes, table, rhs_hi, rhs_lo, full, sems = refs[4:]
    planes = miller.shape[1]
    half = waves.shape[2]
    pairs = (
        (sizes_in, sizes),
        (species_in, species),
        (miller_in, miller),
        (positions_in, positions),
        (form_in, form),
        (waves_in.at[:, :, pl.ds(0, half)], waves),
    )
    copies = [pltpu.make_async_copy(a, b, sems.at[n]) for n, (a, b) in enumerate(pairs)]
    for copy in copies:
        copy.start()
    for copy in copies[:5]:
        copy.wait()
    fill_rows(table, form)
    depth = table.shape[0]
    m = miller[...].astype(F32)
    cosine, sine = trig(positions[...], m)
    cosine, sine = stacked(cosine), stacked(sine)
    radial = stacked(table[...])
    row, owners, _ = rows_by_projector(sizes[...].astype(F32), species[...].astype(F32), form.shape[1])
    picks = hot_rows(row, depth)
    rows = PROJ // 4
    for r in range(4):
        part = slice(r * rows, (r + 1) * rows)
        size = dot(picks[part], radial)
        hi, lo = split(size * dot(owners[part], cosine))
        hi_ref[part, 0:planes] = hi
        lo_ref[part, 0:planes] = lo
        hi, lo = split(-(size * dot(owners[part], sine)))
        hi_ref[part, planes : 2 * planes] = hi
        lo_ref[part, planes : 2 * planes] = lo
    copies[5].wait()
    project_half(order, waves[0], waves[1], m, hi_ref, lo_ref, outs, rhs_hi, rhs_lo, full)


def project_second(order, waves, miller, hi_ref, lo_ref, *refs):
    outs, (rhs_hi, rhs_lo, full) = refs[:2], refs[2:]
    half = waves.shape[2] // 2
    re, im = waves[0, :, half:], waves[1, :, half:]
    project_half(order, re, im, miller[...].astype(F32), hi_ref, lo_ref, outs, rhs_hi, rhs_lo, full)


def apply_tables_kernel(miller, positions, form, coupling, species, sizes, hi_ref, lo_ref, dense_hi, dense_lo, table, ctable):
    planes = miller.shape[1]
    nspec = form.shape[1]
    fill_rows(table, form)
    fill_rows(ctable, coupling)
    depth = table.shape[0]
    m = miller[...].astype(F32)
    cosine, sine = trig(positions[...], m)
    cosine, sine = stacked(cosine), stacked(sine)
    radial = stacked(table[...])
    lengths, kinds = sizes[...].astype(F32), species[...].astype(F32)
    row, owners, owner_row, channel = rows_by_lane(lengths, kinds, nspec)
    picks = hot_rows_t(row, depth)
    step = planes // 4
    over = ((0,), (0,))
    for r in range(4):
        part = slice(r * step, (r + 1) * step)
        size = dot(radial[:, part], picks, over)
        hi, lo = split(size * dot(cosine[:, part], owners, over))
        hi_ref[part, 0:PROJ] = hi
        lo_ref[part, 0:PROJ] = lo
        hi, lo = split(-(size * dot(sine[:, part], owners, over)))
        hi_ref[part, PROJ : 2 * PROJ] = hi
        lo_ref[part, PROJ : 2 * PROJ] = lo
    row, _, owner_col = rows_by_projector(lengths, kinds, nspec)
    lines = dot(hot_rows(row, depth), stacked(ctable[...]))
    lines_hi, lines_lo = split(lines)
    spread = jnp.where(iota((ctable.shape[1], PROJ), 0).astype(F32) == channel, 1.0, 0.0).astype(BF16)
    dense = dot(lines_hi, spread) + dot(lines_lo, spread)
    hi, lo = split(jnp.where(owner_col == owner_row, dense, 0.0))
    dense_hi[...] = hi
    dense_lo[...] = lo


def stats_kernel(order, own, near, far, sums, occupation, dense_hi, dense_lo, *refs):
    share_in, levels_in = refs[:-5] or (None, None)
    rhs_hi, rhs_lo, level_out, share_out, full = refs[-5:]
    rows = PROJ // 4
    half = occupation.shape[1]
    device = lax.axis_index("ga")
    for rel, ref, at in (((0, 0), own, 0), ((0, 1), near, 0), ((1, 0), far, 0), ((1, 1), far, rows)):
        full[pl.ds(block_row(device, order, rel, rows), rows)] = ref[at : at + rows]
    proj = full[...]
    p_hi, p_lo = split(proj)
    mixed = dot(dense_hi[...], p_hi) + dot(dense_hi[...], p_lo) + dot(dense_lo[...], p_hi)
    pairs = jnp.sum(proj * mixed, axis=0, keepdims=True)
    nonlocal_sum = pairs[:, 0:half] + pairs[:, half:]
    kin, norm = sums[0:1, 0:half], sums[1:2, 0:half]
    level = (kin + nonlocal_sum) / (norm + EPSILON)
    share = jnp.sum(occupation[...] * (nonlocal_sum / (norm + EPSILON)), axis=1, keepdims=True)
    if share_in is None:
        level_out[...] = level
        share_out[...] = share
    else:
        level_out[0:1] = levels_in[...]
        level_out[1:2] = level
        share_out[...] = share_in[...] + share
    m_hi, m_lo = split(mixed)
    for ref, m in ((rhs_hi, m_hi), (rhs_lo, m_lo)):
        ref[0:PROJ] = m
        ref[PROJ:, 0:half] = -m[:, half:]
        ref[PROJ:, half:] = m[:, 0:half]


def apply_kernel(q, rhs_hi, rhs_lo, levels, waves, miller, hi_ref, lo_ref, *refs):
    residual, staged, sem = refs[-3:]
    planes = miller.shape[1]
    half = staged.shape[2]
    bands = slice(q * half, (q + 1) * half)
    level = levels[q : q + 1]
    unit = jnp.where(iota((8, half), 0) == 0, 1.0, 0.0).astype(BF16)
    applied = dot(hi_ref[...], rhs_hi[...]) + dot(hi_ref[...], rhs_lo[...]) + dot(lo_ref[...], rhs_hi[...])
    line = jnp.broadcast_to(squares(miller[...].astype(F32)), (8, planes)).astype(BF16)
    shifted = (0.5 * KINETIC_SCALE) * dot(line, unit, ((0,), (0,))) - level
    staged[0] = shifted * waves[0, :, bands] + applied[:, 0:half]
    staged[1] = shifted * waves[1, :, bands] + applied[:, half:]
    copy = pltpu.make_async_copy(staged, residual.at[:, :, pl.ds(q * half, half)], sem)
    copy.start()
    copy.wait()


def swap(x, axis, size, mask):
    return lax.ppermute(x, axis, [(i, i ^ mask) for i in range(size)])


def tree(parts):
    while len(parts) > 1:
        parts = [a + b for a, b in zip(parts[::2], parts[1::2])]
    return parts[0]


def on_device(ga, band, waves, miller, positions, form_factors, coupling, species, block_sizes, occupation):
    _, planes, bands = waves.shape
    half = bands // 2
    nspec, kmax, _ = form_factors.shape
    atoms = species.shape[0]
    rows = PROJ // 4
    depth = depth_of(kmax, nspec)
    positions = positions.T
    form = form_factors.transpose(1, 0, 2)
    coupling = coupling.transpose(1, 0, 2)
    species = species.reshape(1, -1)
    sizes = block_sizes.reshape(1, -1)
    bits = ga.bit_length() - 1
    orders = ((0, 1), (1, 0))
    params = pltpu.CompilerParams(vmem_limit_bytes=32 * 1024 * 1024)
    hbm = pl.BlockSpec(memory_space=pltpu.HBM)
    vmem = pl.BlockSpec(memory_space=pltpu.VMEM)
    shape = jax.ShapeDtypeStruct
    pieces = [shape((2 * rows + 8, bands), F32)] * 2
    beta = [shape((PROJ, 2 * planes), BF16)] * 2
    work = [
        pltpu.VMEM((2 * planes, bands), BF16),
        pltpu.VMEM((2 * planes, bands), BF16),
        pltpu.VMEM((PROJ, bands), F32),
    ]
    out = pl.pallas_call(
        functools.partial(project_first, orders[0]),
        name="project_first",
        in_specs=[hbm] * 6,
        out_shape=pieces + beta,
        scratch_shapes=[
            pltpu.VMEM((2, planes, half), F32),
            pltpu.VMEM(miller.shape, jnp.int32),
            pltpu.VMEM(positions.shape, F32),
            pltpu.VMEM(form.shape, F32),
            pltpu.VMEM((1, atoms), jnp.int32),
            pltpu.VMEM((1, atoms), jnp.int32),
            pltpu.VMEM((depth, planes), F32),
            *work,
            pltpu.SemaphoreType.DMA((6,)),
        ],
        compiler_params=params,
    )(*(pltpu.with_memory_space_constraint(x, pltpu.HBM) for x in (waves, miller, positions, form, species, sizes)))
    parts = [out[:2]]
    parts.append(
        pl.pallas_call(
            functools.partial(project_second, orders[1]),
            name="project_second",
            out_shape=pieces,
            scratch_shapes=work,
            compiler_params=params,
        )(waves, miller, out[2], out[3])
    )
    tables = pl.pallas_call(
        apply_tables_kernel,
        name="apply_tables",
        out_shape=[shape((planes, 2 * PROJ), BF16)] * 2 + [shape((PROJ, PROJ), BF16)] * 2,
        scratch_shapes=[pltpu.VMEM((depth, planes), F32), pltpu.VMEM((depth, LANES), F32)],
        compiler_params=params,
    )(miller, positions, form, coupling, species, sizes)
    kept, mine, own, near, far = {}, {}, {}, {}, {}
    for q, order in enumerate(orders):
        kept[q] = parts[q][1] + swap(parts[q][0], "ga", ga, 1 << order[0])
    for q, order in enumerate(orders):
        k = kept[q]
        got = swap(k[rows:], "ga", ga, 1 << order[1])
        mine[q] = jnp.concatenate([k[:rows] + got[:rows], k[2 * rows :] + got[rows:]], axis=0)
    for b in range(2, bits):
        for q in range(2):
            mine[q] = mine[q] + swap(mine[q], "ga", ga, 1 << b)
    for q, order in enumerate(orders):
        own[q] = mine[q][:rows]
        near[q] = swap(own[q], "ga", ga, 1 << order[1])
    for q, order in enumerate(orders):
        far[q] = swap(jnp.concatenate([own[q], near[q]], axis=0), "ga", ga, 1 << order[0])
    occ = occupation.reshape(2, half)
    residual = levels = share = None
    for q in range(2):
        operands = [own[q], near[q], far[q], mine[q][rows:], occ[q : q + 1], tables[2], tables[3]]
        if q == 1:
            operands += [share, levels]
        rhs_hi, rhs_lo, levels, share = pl.pallas_call(
            functools.partial(stats_kernel, orders[q]),
            out_shape=[
                shape((2 * PROJ, bands), BF16),
                shape((2 * PROJ, bands), BF16),
                shape((q + 1, half), F32),
                shape((1, 1), F32),
            ],
            scratch_shapes=[pltpu.VMEM((PROJ, bands), F32)],
            compiler_params=params,
        )(*operands)
        if q == 1:
            energy = tree([share] + [swap(share, "band", band, d) for d in range(1, band)])
        operands = [rhs_hi, rhs_lo, levels, waves, miller, tables[0], tables[1]]
        specs = [vmem] * len(operands)
        alias = {}
        if q == 1:
            alias = {len(operands): 0}
            operands.append(residual)
            specs.append(hbm)
        residual = pl.pallas_call(
            functools.partial(apply_kernel, q),
            in_specs=specs,
            out_specs=hbm,
            out_shape=shape(waves.shape, F32),
            scratch_shapes=[pltpu.VMEM((2, planes, half), F32), pltpu.SemaphoreType.DMA],
            input_output_aliases=alias,
            compiler_params=params,
        )(*operands)
    return residual, levels.reshape(bands), energy.reshape(())


def solution(mesh):
    in_specs = (
        P(None, "ga", "band"),
        P(None, "ga"),
        P(),
        P(None, None, "ga"),
        P(),
        P(),
        P(),
        P("band"),
    )
    out_specs = (P(None, "ga", "band"), P("band"), P())

    def body(*args):
        return on_device(mesh.shape["ga"], mesh.shape["band"], *args)

    return jax.shard_map(body, mesh=mesh, in_specs=in_specs, out_specs=out_specs, check_vma=False)
```

```python
import functools
import math

import jax
import jax.numpy as jnp
from jax import lax
from jax.experimental import pallas as pl
from jax.experimental.pallas import tpu as pltpu
from jax.sharding import PartitionSpec as P

PROJ = 512
KINETIC_SCALE = 0.005
EPSILON = 1e-06
LANES = 128
F32 = jnp.float32
BF16 = jnp.bfloat16


def iota(shape, dim):
    return lax.broadcasted_iota(jnp.int32, shape, dim)


def split(x):
    hi = x.astype(BF16)
    return hi, (x - hi.astype(F32)).astype(BF16)


def dot(a, b, contract=((1,), (0,))):
    return lax.dot_general(a, b, (contract, ((), ())), preferred_element_type=F32)


def pick(mask, values, axis):
    return jnp.sum(jnp.where(mask, values, 0.0), axis=axis, keepdims=True)


def depth_of(kmax, nspec):
    return -(-kmax * nspec // 16) * 16


def columns_of(sizes, species):
    atoms = sizes.shape[1]
    here, there = iota((atoms, atoms), 0), iota((atoms, atoms), 1)
    start = pick(there < here, sizes, 1)
    size = pick(there == here, sizes, 1)
    spec = pick(there == here, species, 1)
    return start, size, spec


def rows_by_projector(sizes, species, nspec):
    atoms = sizes.shape[1]
    _, size, spec = columns_of(sizes, species)
    atom = lax.rem(iota((atoms, 2 * atoms), 1), atoms)
    here = iota((atoms, 2 * atoms), 0)
    start = pick(here < atom, size, 0)
    end = start + pick(here == atom, size, 0)
    spec = pick(here == atom, spec, 0)
    place = iota((PROJ, 2 * atoms), 0).astype(F32)
    hot = (place >= start) & (place < end)
    lane = iota((PROJ, 2 * atoms), 1)
    first = hot & (lane < atoms)
    row = pick(first, spec - nspec * start, 1) + nspec * iota((PROJ, 1), 0).astype(F32)
    owner = pick(first, lane.astype(F32), 1)
    return row, jnp.where(hot, 1.0, 0.0).astype(BF16), owner


def rows_by_lane(sizes, species, nspec):
    atoms = sizes.shape[1]
    start, size, spec = columns_of(sizes, species)
    place = iota((atoms, PROJ), 1).astype(F32)
    hot = (place >= start) & (place < start + size)
    lane = iota((1, PROJ), 1).astype(F32)
    channel = lane - pick(hot, start, 0)
    row = nspec * channel + pick(hot, spec, 0)
    owner = pick(hot, iota((atoms, PROJ), 0).astype(F32), 0)
    ones = jnp.where(hot, 1.0, 0.0)
    return row, jnp.concatenate([ones, ones], axis=0).astype(BF16), owner, channel


def column(rows, n):
    size = rows.shape[1]
    return pick(iota((size, size), 0) == iota((size, size), 1), rows[n : n + 1], 1)


def trig(positions, miller):
    cycles = (
        column(positions, 0) * miller[0:1] + column(positions, 1) * miller[1:2] + column(positions, 2) * miller[2:3]
    )
    half = (cycles - jnp.round(cycles)) * math.pi
    sq = half * half
    sine = 1.0 / 6227020800.0
    for n in (39916800.0, 362880.0, 5040.0, 120.0, 6.0, 1.0):
        sine = 1.0 / n - sq * sine
    sine = half * sine
    cosine = 1.0 / 479001600.0
    for n in (3628800.0, 40320.0, 720.0, 24.0, 2.0, 1.0):
        cosine = 1.0 / n - sq * cosine
    return 1.0 - 2.0 * sine * sine, 2.0 * sine * cosine


def stacked(x):
    hi, lo = split(x)
    return jnp.concatenate([hi, lo], axis=0)


def fill_rows(scratch, table):
    kmax, nspec, width = table.shape
    scratch[...] = jnp.zeros(scratch.shape, F32)
    for k in range(kmax):
        scratch[k * nspec : (k + 1) * nspec, 0:width] = table[k]


def hot_rows(row, depth):
    j = lax.rem(iota((PROJ, 2 * depth), 1), depth).astype(F32)
    return jnp.where(row == j, 1.0, 0.0).astype(BF16)


def hot_rows_t(row, depth):
    j = lax.rem(iota((2 * depth, PROJ), 0), depth).astype(F32)
    return jnp.where(row == j, 1.0, 0.0).astype(BF16)


def squares(miller):
    total = miller[0:1] * miller[0:1] + miller[1:2] * miller[1:2] + miller[2:3] * miller[2:3]
    return total


def bit(device, b):
    return lax.rem(lax.shift_right_logical(device, b), 2)


def block_row(device, order, rel, rows):
    index = 2 * lax.bitwise_xor(bit(device, order[0]), rel[0]) + lax.bitwise_xor(bit(device, order[1]), rel[1])
    return pl.multiple_of(index * rows, rows)


def half_row(device, order, rel, rows):
    return pl.multiple_of(lax.bitwise_xor(bit(device, order[0]), rel) * 2 * rows, rows)


def load_bands(re, im, rhs_hi, rhs_lo):
    planes, half = re.shape
    re_hi, re_lo = split(re)
    im_hi, im_lo = split(im)
    for ref, a, b in ((rhs_hi, re_hi, im_hi), (rhs_lo, re_lo, im_lo)):
        ref[0:planes, 0:half] = a
        ref[0:planes, half:] = b
        ref[planes:, 0:half] = b
        ref[planes:, half:] = -a


def band_sums(re, im, miller):
    planes, half = re.shape
    weight = jnp.where(iota((8, planes), 0) == 0, squares(miller), 1.0).astype(BF16)
    scale = jnp.where(iota((8, half), 0) == 0, 0.5 * KINETIC_SCALE, 1.0)
    hi, lo = split(re * re + im * im)
    return scale * (dot(weight, hi) + dot(weight, lo))


def beta_rows(at, count, picks, owners, cosine, sine, radial, hi_ref, lo_ref):
    planes = cosine.shape[1]
    step = count // 2
    for r in range(2):
        source = pl.ds(pl.multiple_of(at + r * step, step), step)
        part = slice(r * step, (r + 1) * step)
        owner = owners[source]
        size = dot(picks[source], radial[...])
        hi, lo = split(size * dot(owner, cosine[...]))
        hi_ref[part, 0:planes] = hi
        lo_ref[part, 0:planes] = lo
        hi, lo = split(-(size * dot(owner, sine[...])))
        hi_ref[part, planes : 2 * planes] = hi
        lo_ref[part, planes : 2 * planes] = lo


def project(hi_ref, lo_ref, rhs_hi, rhs_lo):
    return dot(hi_ref[...], rhs_hi[...]) + dot(hi_ref[...], rhs_lo[...]) + dot(lo_ref[...], rhs_hi[...])


def ordered(device, order, full, out):
    rows = full.shape[0] // 2
    for second in (0, 1):
        at = pl.multiple_of(lax.bitwise_xor(bit(device, order[1]), second) * rows, rows)
        out[second * rows : (second + 1) * rows] = full[pl.ds(at, rows)]


def project_send(order, waves_in, miller_in, positions_in, form_in, species_in, sizes_in, *refs):
    out, hi_ref, lo_ref, rhs_hi, rhs_lo, cosine, sine, radial, picks, owners = refs[:10]
    waves, miller, positions, form, species, sizes, table, full, sems = refs[10:]
    half = waves.shape[2]
    pairs = (
        (sizes_in, sizes),
        (species_in, species),
        (miller_in, miller),
        (positions_in, positions),
        (form_in, form),
        (waves_in.at[:, :, pl.ds(0, half)], waves),
    )
    copies = [pltpu.make_async_copy(a, b, sems.at[n]) for n, (a, b) in enumerate(pairs)]
    for copy in copies:
        copy.start()
    device = lax.axis_index("ga")
    for copy in copies[:5]:
        copy.wait()
    fill_rows(table, form)
    cos, sin = trig(positions[...], miller[...].astype(F32))
    cosine[...] = stacked(cos)
    sine[...] = stacked(sin)
    radial[...] = stacked(table[...])
    row, owner, _ = rows_by_projector(sizes[...].astype(F32), species[...].astype(F32), form.shape[1])
    picks[...] = hot_rows(row, table.shape[0])
    owners[...] = owner
    rows = PROJ // 4
    beta_rows(half_row(device, order, 1, rows), 2 * rows, picks, owners, cosine, sine, radial, hi_ref, lo_ref)
    copies[5].wait()
    load_bands(waves[0], waves[1], rhs_hi, rhs_lo)
    full[...] = project(hi_ref, lo_ref, rhs_hi, rhs_lo)
    ordered(device, order, full, out)


def project_rest(order, waves, miller, hi_ref, lo_ref, rhs_hi, rhs_lo, cosine, sine, radial, picks, owners, *refs):
    keep_first, send_second, keep_second, hi_keep, lo_keep, rhs_hi2, rhs_lo2, full = refs
    half = waves.shape[2] // 2
    rows = PROJ // 4
    device = lax.axis_index("ga")
    beta_rows(half_row(device, order, 0, rows), 2 * rows, picks, owners, cosine, sine, radial, hi_keep, lo_keep)
    full[...] = project(hi_keep, lo_keep, rhs_hi, rhs_lo)
    ordered(device, order, full, keep_first)
    load_bands(waves[0, :, half:], waves[1, :, half:], rhs_hi2, rhs_lo2)
    m = miller[...].astype(F32)
    sums = [band_sums(waves[0, :, part], waves[1, :, part], m) for part in (slice(0, half), slice(half, 2 * half))]
    tail = jnp.concatenate(sums, axis=1)
    for hi, lo, out in ((hi_ref, lo_ref, send_second), (hi_keep, lo_keep, keep_second)):
        full[...] = project(hi, lo, rhs_hi2, rhs_lo2)
        ordered(device, order, full, out)
        out[2 * rows :] = tail


def apply_tables_kernel(miller, positions, form, coupling, species, sizes, hi_ref, lo_ref, dense_hi, dense_lo, table, ctable):
    planes = miller.shape[1]
    nspec = form.shape[1]
    fill_rows(table, form)
    fill_rows(ctable, coupling)
    depth = table.shape[0]
    m = miller[...].astype(F32)
    cosine, sine = trig(positions[...], m)
    cosine, sine = stacked(cosine), stacked(sine)
    radial = stacked(table[...])
    lengths, kinds = sizes[...].astype(F32), species[...].astype(F32)
    row, owners, owner_row, channel = rows_by_lane(lengths, kinds, nspec)
    picks = hot_rows_t(row, depth)
    step = planes // 4
    over = ((0,), (0,))
    for r in range(4):
        part = slice(r * step, (r + 1) * step)
        size = dot(radial[:, part], picks, over)
        hi, lo = split(size * dot(cosine[:, part], owners, over))
        hi_ref[part, 0:PROJ] = hi
        lo_ref[part, 0:PROJ] = lo
        hi, lo = split(-(size * dot(sine[:, part], owners, over)))
        hi_ref[part, PROJ : 2 * PROJ] = hi
        lo_ref[part, PROJ : 2 * PROJ] = lo
    row, _, owner_col = rows_by_projector(lengths, kinds, nspec)
    lines = dot(hot_rows(row, depth), stacked(ctable[...]))
    lines_hi, lines_lo = split(lines)
    spread = jnp.where(iota((ctable.shape[1], PROJ), 0).astype(F32) == channel, 1.0, 0.0).astype(BF16)
    dense = dot(lines_hi, spread) + dot(lines_lo, spread)
    hi, lo = split(jnp.where(owner_col == owner_row, dense, 0.0))
    dense_hi[...] = hi
    dense_lo[...] = lo


def stats_kernel(order, q, own, near, far, sums, occupation, dense_hi, dense_lo, *refs):
    rhs_hi, rhs_lo, level_out, share_out, full = refs[-5:]
    rows = PROJ // 4
    half = occupation.shape[1]
    bands = slice(q * half, (q + 1) * half)
    device = lax.axis_index("ga")
    for rel, ref, at in (((0, 0), own, 0), ((0, 1), near, 0), ((1, 0), far, 0), ((1, 1), far, rows)):
        full[pl.ds(block_row(device, order, rel, rows), rows)] = ref[at : at + rows]
    proj = full[...]
    p_hi, p_lo = split(proj)
    mixed = dot(dense_hi[...], p_hi) + dot(dense_hi[...], p_lo) + dot(dense_lo[...], p_hi)
    pairs = jnp.sum(proj * mixed, axis=0, keepdims=True)
    nonlocal_sum = pairs[:, 0:half] + pairs[:, half:]
    kin, norm = sums[0:1, bands], sums[1:2, bands]
    level_out[...] = (kin + nonlocal_sum) / (norm + EPSILON)
    share = jnp.sum(occupation[...] * (nonlocal_sum / (norm + EPSILON)), axis=1, keepdims=True)
    share = jnp.broadcast_to(share, share_out.shape)
    for other in refs[:-5]:
        share = other[...] + share
    share_out[...] = share
    m_hi, m_lo = split(mixed)
    for ref, m in ((rhs_hi, m_hi), (rhs_lo, m_lo)):
        ref[0:PROJ] = m
        ref[PROJ:, 0:half] = -m[:, half:]
        ref[PROJ:, half:] = m[:, 0:half]


def apply_kernel(q, rhs_hi, rhs_lo, waves, miller, hi_ref, lo_ref, level, *refs):
    planes = miller.shape[1]
    half = level.shape[1]
    bands = slice(q * half, (q + 1) * half)
    unit = jnp.where(iota((8, half), 0) == 0, 1.0, 0.0).astype(BF16)
    applied = dot(hi_ref[...], rhs_hi[...]) + dot(hi_ref[...], rhs_lo[...]) + dot(lo_ref[...], rhs_hi[...])
    line = jnp.broadcast_to(squares(miller[...].astype(F32)), (8, planes)).astype(BF16)
    shifted = (0.5 * KINETIC_SCALE) * dot(line, unit, ((0,), (0,))) - level[...]
    if q == 0:
        residual, staged, sems = refs
    else:
        before, _, residual, estimate, staged, levels, sems = refs
        levels[0:1] = before[...]
        levels[1:2] = level[...]
    staged[0] = shifted * waves[0, :, bands] + applied[:, 0:half]
    staged[1] = shifted * waves[1, :, bands] + applied[:, half:]
    copies = [pltpu.make_async_copy(staged, residual.at[:, :, pl.ds(q * half, half)], sems.at[0])]
    if q == 1:
        copies.append(pltpu.make_async_copy(levels, estimate, sems.at[1]))
    for copy in copies:
        copy.start()
    for copy in copies:
        copy.wait()


def swap(x, axis, size, mask):
    return lax.ppermute(x, axis, [(i, i ^ mask) for i in range(size)])


def tree(parts):
    while len(parts) > 1:
        parts = [a + b for a, b in zip(parts[::2], parts[1::2])]
    return parts[0]


def on_device(ga, band, waves, miller, positions, form_factors, coupling, species, block_sizes, occupation):
    _, planes, bands = waves.shape
    half = bands // 2
    nspec, kmax, _ = form_factors.shape
    atoms = species.shape[0]
    rows = PROJ // 4
    depth = depth_of(kmax, nspec)
    positions = positions.T
    form = form_factors.transpose(1, 0, 2)
    coupling = coupling.transpose(1, 0, 2)
    species = species.reshape(1, -1)
    sizes = block_sizes.reshape(1, -1)
    bits = ga.bit_length() - 1
    order = (0, 1)
    params = pltpu.CompilerParams(vmem_limit_bytes=32 * 1024 * 1024)
    hbm = pl.BlockSpec(memory_space=pltpu.HBM)
    vmem = pl.BlockSpec(memory_space=pltpu.VMEM)
    shape = jax.ShapeDtypeStruct
    plain, summed = shape((2 * rows, bands), F32), shape((2 * rows + 8, bands), F32)
    beta = [((2 * rows, 2 * planes), BF16)] * 2
    rhs = [((2 * planes, bands), BF16)] * 2
    tables = [((2 * atoms, planes), BF16)] * 2 + [((2 * depth, planes), BF16), ((PROJ, 2 * depth), BF16), ((PROJ, 2 * atoms), BF16)]
    send_first, *passed = pl.pallas_call(
        functools.partial(project_send, order),
        name="project_send",
        in_specs=[hbm] * 6,
        out_shape=[plain] + [shape(*x) for x in beta + rhs + tables],
        scratch_shapes=[
            pltpu.VMEM((2, planes, half), F32),
            pltpu.VMEM(miller.shape, jnp.int32),
            pltpu.VMEM(positions.shape, F32),
            pltpu.VMEM(form.shape, F32),
            pltpu.VMEM((1, atoms), jnp.int32),
            pltpu.VMEM((1, atoms), jnp.int32),
            pltpu.VMEM((depth, planes), F32),
            pltpu.VMEM((2 * rows, bands), F32),
            pltpu.SemaphoreType.DMA((6,)),
        ],
        compiler_params=params,
    )(*(pltpu.with_memory_space_constraint(x, pltpu.HBM) for x in (waves, miller, positions, form, species, sizes)))
    keep_first, send_second, keep_second = pl.pallas_call(
        functools.partial(project_rest, order),
        name="project_rest",
        out_shape=[plain, summed, summed],
        scratch_shapes=[pltpu.VMEM(*x) for x in beta + rhs] + [pltpu.VMEM((2 * rows, bands), F32)],
        compiler_params=params,
    )(waves, miller, *passed)
    tables = pl.pallas_call(
        apply_tables_kernel,
        name="apply_tables",
        out_shape=[shape((planes, 2 * PROJ), BF16)] * 2 + [shape((PROJ, PROJ), BF16)] * 2,
        scratch_shapes=[pltpu.VMEM((depth, planes), F32), pltpu.VMEM((depth, LANES), F32)],
        compiler_params=params,
    )(miller, positions, form, coupling, species, sizes)
    mine, own, near, far = {}, {}, {}, {}
    kept = [
        keep_first + swap(send_first, "ga", ga, 1 << order[0]), keep_second + swap(send_second, "ga", ga, 1 << order[0])
    ]
    for q, k in enumerate(kept):
        got = swap(k[rows:], "ga", ga, 1 << order[1])
        mine[q] = k[:rows] + got[:rows]
        if q == 1:
            mine[q] = jnp.concatenate([mine[q], k[2 * rows :] + got[rows:]], axis=0)
    for b in range(2, bits):
        for q in range(2):
            mine[q] = mine[q] + swap(mine[q], "ga", ga, 1 << b)
    for q in range(2):
        own[q] = mine[q][:rows]
        near[q] = swap(own[q], "ga", ga, 1 << order[1])
    for q in range(2):
        far[q] = swap(jnp.concatenate([own[q], near[q]], axis=0), "ga", ga, 1 << order[0])
    sums = mine[1][rows:]
    occ = occupation.reshape(2, half)
    residual, levels, share = [], [], []
    for q in range(2):
        rhs_hi, rhs_lo, level, total = pl.pallas_call(
            functools.partial(stats_kernel, order, q),
            out_shape=[shape((2 * PROJ, bands), BF16)] * 2 + [shape((1, half), F32)] * 2,
            scratch_shapes=[pltpu.VMEM((PROJ, bands), F32)],
            compiler_params=params,
        )(own[q], near[q], far[q], sums, occ[q : q + 1], tables[2], tables[3], *share)
        share = [total]
        if q == 1:
            energy = tree([total] + [swap(total, "band", band, d) for d in range(1, band)])[0, 0]
        operands = [rhs_hi, rhs_lo, waves, miller, tables[0], tables[1], level, *levels, *residual]
        levels.append(level)
        residual = pl.pallas_call(
            functools.partial(apply_kernel, q),
            in_specs=[vmem] * (7 + q) + [hbm] * q,
            out_specs=[hbm] * (1 + q),
            out_shape=[shape(waves.shape, F32)] + [shape((2, half), F32)] * q,
            scratch_shapes=[pltpu.VMEM((2, planes, half), F32)]
            + [pltpu.VMEM((2, half), F32)] * q
            + [pltpu.SemaphoreType.DMA((2,))],
            input_output_aliases={8: 0} if q else {},
            compiler_params=params,
        )(*operands)
    return residual[0], residual[1].reshape(bands), energy


def solution(mesh):
    in_specs = (
        P(None, "ga", "band"),
        P(None, "ga"),
        P(),
        P(None, None, "ga"),
        P(),
        P(),
        P(),
        P("band"),
    )
    out_specs = (P(None, "ga", "band"), P("band"), P())

    def body(*args):
        return on_device(mesh.shape["ga"], mesh.shape["band"], *args)

    return jax.shard_map(body, mesh=mesh, in_specs=in_specs, out_specs=out_specs, check_vma=False)
```

```python
import functools
import math

import jax
import jax.numpy as jnp
from jax import lax
from jax.experimental import pallas as pl
from jax.experimental.pallas import tpu as pltpu
from jax.sharding import PartitionSpec as P

PROJ = 512
KINETIC_SCALE = 0.005
EPSILON = 1e-06
LANES = 128
F32 = jnp.float32
BF16 = jnp.bfloat16


def iota(shape, dim):
    return lax.broadcasted_iota(jnp.int32, shape, dim)


def split(x):
    hi = x.astype(BF16)
    return hi, (x - hi.astype(F32)).astype(BF16)


def dot(a, b, contract=((1,), (0,))):
    return lax.dot_general(a, b, (contract, ((), ())), preferred_element_type=F32)


def pick(mask, values, axis):
    return jnp.sum(jnp.where(mask, values, 0.0), axis=axis, keepdims=True)


def depth_of(kmax, nspec):
    return -(-kmax * nspec // 16) * 16


def columns_of(sizes, species):
    atoms = sizes.shape[1]
    here, there = iota((atoms, atoms), 0), iota((atoms, atoms), 1)
    start = pick(there < here, sizes, 1)
    size = pick(there == here, sizes, 1)
    spec = pick(there == here, species, 1)
    return start, size, spec


def rows_by_projector(sizes, species, nspec):
    atoms = sizes.shape[1]
    _, size, spec = columns_of(sizes, species)
    atom = lax.rem(iota((atoms, 2 * atoms), 1), atoms)
    here = iota((atoms, 2 * atoms), 0)
    start = pick(here < atom, size, 0)
    end = start + pick(here == atom, size, 0)
    spec = pick(here == atom, spec, 0)
    place = iota((PROJ, 2 * atoms), 0).astype(F32)
    hot = (place >= start) & (place < end)
    lane = iota((PROJ, 2 * atoms), 1)
    first = hot & (lane < atoms)
    row = pick(first, spec - nspec * start, 1) + nspec * iota((PROJ, 1), 0).astype(F32)
    owner = pick(first, lane.astype(F32), 1)
    return row, jnp.where(hot, 1.0, 0.0).astype(BF16), owner


def rows_by_lane(sizes, species, nspec):
    atoms = sizes.shape[1]
    start, size, spec = columns_of(sizes, species)
    place = iota((atoms, PROJ), 1).astype(F32)
    hot = (place >= start) & (place < start + size)
    lane = iota((1, PROJ), 1).astype(F32)
    channel = lane - pick(hot, start, 0)
    row = nspec * channel + pick(hot, spec, 0)
    owner = pick(hot, iota((atoms, PROJ), 0).astype(F32), 0)
    ones = jnp.where(hot, 1.0, 0.0)
    return row, jnp.concatenate([ones, ones], axis=0).astype(BF16), owner, channel


def column(rows, n):
    size = rows.shape[1]
    return pick(iota((size, size), 0) == iota((size, size), 1), rows[n : n + 1], 1)


def trig(positions, miller):
    cycles = (
        column(positions, 0) * miller[0:1] + column(positions, 1) * miller[1:2] + column(positions, 2) * miller[2:3]
    )
    half = (cycles - jnp.round(cycles)) * math.pi
    sq = half * half
    sine = 1.0 / 6227020800.0
    for n in (39916800.0, 362880.0, 5040.0, 120.0, 6.0, 1.0):
        sine = 1.0 / n - sq * sine
    sine = half * sine
    cosine = 1.0 / 479001600.0
    for n in (3628800.0, 40320.0, 720.0, 24.0, 2.0, 1.0):
        cosine = 1.0 / n - sq * cosine
    return 1.0 - 2.0 * sine * sine, 2.0 * sine * cosine


def stacked(x):
    hi, lo = split(x)
    return jnp.concatenate([hi, lo], axis=0)


def fill_rows(scratch, table):
    kmax, nspec, width = table.shape
    scratch[...] = jnp.zeros(scratch.shape, F32)
    for k in range(kmax):
        scratch[k * nspec : (k + 1) * nspec, 0:width] = table[k]


def hot_rows(row, depth):
    j = lax.rem(iota((PROJ, 2 * depth), 1), depth).astype(F32)
    return jnp.where(row == j, 1.0, 0.0).astype(BF16)


def hot_rows_t(row, depth):
    j = lax.rem(iota((2 * depth, PROJ), 0), depth).astype(F32)
    return jnp.where(row == j, 1.0, 0.0).astype(BF16)


def squares(miller):
    total = miller[0:1] * miller[0:1] + miller[1:2] * miller[1:2] + miller[2:3] * miller[2:3]
    return total


def bit(device, b):
    return lax.rem(lax.shift_right_logical(device, b), 2)


def block_row(device, order, rel, rows):
    index = 2 * lax.bitwise_xor(bit(device, order[0]), rel[0]) + lax.bitwise_xor(bit(device, order[1]), rel[1])
    return pl.multiple_of(index * rows, rows)


def half_row(device, order, rel, rows):
    return pl.multiple_of(lax.bitwise_xor(bit(device, order[0]), rel) * 2 * rows, rows)


def load_bands(re, im, rhs_hi, rhs_lo):
    planes, half = re.shape
    re_hi, re_lo = split(re)
    im_hi, im_lo = split(im)
    for ref, a, b in ((rhs_hi, re_hi, im_hi), (rhs_lo, re_lo, im_lo)):
        ref[0:planes, 0:half] = a
        ref[0:planes, half:] = b
        ref[planes:, 0:half] = b
        ref[planes:, half:] = -a


def band_sums(re, im, miller):
    planes, half = re.shape
    weight = jnp.where(iota((8, planes), 0) == 0, squares(miller), 1.0).astype(BF16)
    scale = jnp.where(iota((8, half), 0) == 0, 0.5 * KINETIC_SCALE, 1.0)
    hi, lo = split(re * re + im * im)
    return scale * (dot(weight, hi) + dot(weight, lo))


def beta_rows(at, count, picks, owners, cosine, sine, radial, hi_ref, lo_ref):
    planes = cosine.shape[1]
    step = count // 2
    for r in range(2):
        source = pl.ds(pl.multiple_of(at + r * step, step), step)
        part = slice(r * step, (r + 1) * step)
        owner = owners[source]
        size = dot(picks[source], radial[...])
        hi, lo = split(size * dot(owner, cosine[...]))
        hi_ref[part, 0:planes] = hi
        lo_ref[part, 0:planes] = lo
        hi, lo = split(-(size * dot(owner, sine[...])))
        hi_ref[part, planes : 2 * planes] = hi
        lo_ref[part, planes : 2 * planes] = lo


def project(hi_ref, lo_ref, rhs_hi, rhs_lo):
    return dot(hi_ref[...], rhs_hi[...]) + dot(hi_ref[...], rhs_lo[...]) + dot(lo_ref[...], rhs_hi[...])


def ordered(device, order, full, outs):
    rows = full.shape[0] // 2
    for second, out in enumerate(outs):
        at = pl.multiple_of(lax.bitwise_xor(bit(device, order[1]), second) * rows, rows)
        out[0:rows] = full[pl.ds(at, rows)]


def project_send(order, waves_in, miller_in, positions_in, form_in, species_in, sizes_in, *refs):
    outs, (hi_ref, lo_ref, rhs_hi, rhs_lo, cosine, sine, radial, picks, owners) = refs[:2], refs[2:11]
    waves, miller, positions, form, species, sizes, table, full, sems = refs[11:]
    half = waves.shape[2]
    pairs = (
        (sizes_in, sizes),
        (species_in, species),
        (miller_in, miller),
        (positions_in, positions),
        (form_in, form),
        (waves_in.at[:, :, pl.ds(0, half)], waves),
    )
    copies = [pltpu.make_async_copy(a, b, sems.at[n]) for n, (a, b) in enumerate(pairs)]
    for copy in copies:
        copy.start()
    device = lax.axis_index("ga")
    for copy in copies[:5]:
        copy.wait()
    fill_rows(table, form)
    cos, sin = trig(positions[...], miller[...].astype(F32))
    cosine[...] = stacked(cos)
    sine[...] = stacked(sin)
    radial[...] = stacked(table[...])
    row, owner, _ = rows_by_projector(sizes[...].astype(F32), species[...].astype(F32), form.shape[1])
    picks[...] = hot_rows(row, table.shape[0])
    owners[...] = owner
    rows = PROJ // 4
    beta_rows(half_row(device, order, 1, rows), 2 * rows, picks, owners, cosine, sine, radial, hi_ref, lo_ref)
    copies[5].wait()
    load_bands(waves[0], waves[1], rhs_hi, rhs_lo)
    full[...] = project(hi_ref, lo_ref, rhs_hi, rhs_lo)
    ordered(device, order, full, outs)


def project_rest(order, waves, miller, hi_ref, lo_ref, rhs_hi, rhs_lo, cosine, sine, radial, picks, owners, *refs):
    first, second_send, second_keep = refs[:2], refs[2:4], refs[4:6]
    hi_keep, lo_keep, rhs_hi2, rhs_lo2, full = refs[6:]
    half = waves.shape[2] // 2
    rows = PROJ // 4
    device = lax.axis_index("ga")
    beta_rows(half_row(device, order, 0, rows), 2 * rows, picks, owners, cosine, sine, radial, hi_keep, lo_keep)
    full[...] = project(hi_keep, lo_keep, rhs_hi, rhs_lo)
    ordered(device, order, full, first)
    load_bands(waves[0, :, half:], waves[1, :, half:], rhs_hi2, rhs_lo2)
    m = miller[...].astype(F32)
    sums = [band_sums(waves[0, :, part], waves[1, :, part], m) for part in (slice(0, half), slice(half, 2 * half))]
    tail = jnp.concatenate(sums, axis=1)
    for hi, lo, outs in ((hi_ref, lo_ref, second_send), (hi_keep, lo_keep, second_keep)):
        full[...] = project(hi, lo, rhs_hi2, rhs_lo2)
        ordered(device, order, full, outs)
        for out in outs:
            out[rows:] = tail


def apply_tables_kernel(miller, positions, form, coupling, species, sizes, hi_ref, lo_ref, dense_hi, dense_lo, table, ctable):
    planes = miller.shape[1]
    nspec = form.shape[1]
    fill_rows(table, form)
    fill_rows(ctable, coupling)
    depth = table.shape[0]
    m = miller[...].astype(F32)
    cosine, sine = trig(positions[...], m)
    cosine, sine = stacked(cosine), stacked(sine)
    radial = stacked(table[...])
    lengths, kinds = sizes[...].astype(F32), species[...].astype(F32)
    row, owners, owner_row, channel = rows_by_lane(lengths, kinds, nspec)
    picks = hot_rows_t(row, depth)
    step = planes // 4
    over = ((0,), (0,))
    for r in range(4):
        part = slice(r * step, (r + 1) * step)
        size = dot(radial[:, part], picks, over)
        hi, lo = split(size * dot(cosine[:, part], owners, over))
        hi_ref[part, 0:PROJ] = hi
        lo_ref[part, 0:PROJ] = lo
        hi, lo = split(-(size * dot(sine[:, part], owners, over)))
        hi_ref[part, PROJ : 2 * PROJ] = hi
        lo_ref[part, PROJ : 2 * PROJ] = lo
    row, _, owner_col = rows_by_projector(lengths, kinds, nspec)
    lines = dot(hot_rows(row, depth), stacked(ctable[...]))
    lines_hi, lines_lo = split(lines)
    spread = jnp.where(iota((ctable.shape[1], PROJ), 0).astype(F32) == channel, 1.0, 0.0).astype(BF16)
    dense = dot(lines_hi, spread) + dot(lines_lo, spread)
    hi, lo = split(jnp.where(owner_col == owner_row, dense, 0.0))
    dense_hi[...] = hi
    dense_lo[...] = lo


def stats_kernel(order, q, own, near, far, across, sums, occupation, dense_hi, dense_lo, *refs):
    rhs_hi, rhs_lo, level_out, share_out, full = refs[-5:]
    rows = PROJ // 4
    half = occupation.shape[1]
    bands = slice(q * half, (q + 1) * half)
    device = lax.axis_index("ga")
    for rel, ref in (((0, 0), own), ((0, 1), near), ((1, 0), far), ((1, 1), across)):
        full[pl.ds(block_row(device, order, rel, rows), rows)] = ref[0:rows]
    proj = full[...]
    p_hi, p_lo = split(proj)
    mixed = dot(dense_hi[...], p_hi) + dot(dense_hi[...], p_lo) + dot(dense_lo[...], p_hi)
    pairs = jnp.sum(proj * mixed, axis=0, keepdims=True)
    nonlocal_sum = pairs[:, 0:half] + pairs[:, half:]
    kin, norm = sums[0:1, bands], sums[1:2, bands]
    level_out[...] = (kin + nonlocal_sum) / (norm + EPSILON)
    share = jnp.sum(occupation[...] * (nonlocal_sum / (norm + EPSILON)), axis=1, keepdims=True)
    share = jnp.broadcast_to(share, share_out.shape)
    for other in refs[:-5]:
        share = other[...] + share
    share_out[...] = share
    m_hi, m_lo = split(mixed)
    for ref, m in ((rhs_hi, m_hi), (rhs_lo, m_lo)):
        ref[0:PROJ] = m
        ref[PROJ:, 0:half] = -m[:, half:]
        ref[PROJ:, half:] = m[:, 0:half]


def apply_kernel(q, rhs_hi, rhs_lo, waves, miller, hi_ref, lo_ref, level, *refs):
    planes = miller.shape[1]
    half = level.shape[1]
    bands = slice(q * half, (q + 1) * half)
    unit = jnp.where(iota((8, half), 0) == 0, 1.0, 0.0).astype(BF16)
    applied = dot(hi_ref[...], rhs_hi[...]) + dot(hi_ref[...], rhs_lo[...]) + dot(lo_ref[...], rhs_hi[...])
    line = jnp.broadcast_to(squares(miller[...].astype(F32)), (8, planes)).astype(BF16)
    shifted = (0.5 * KINETIC_SCALE) * dot(line, unit, ((0,), (0,))) - level[...]
    if q == 0:
        residual, staged, sems = refs
    else:
        before, _, residual, estimate, staged, levels, sems = refs
        levels[0:1] = before[...]
        levels[1:2] = level[...]
    staged[0] = shifted * waves[0, :, bands] + applied[:, 0:half]
    staged[1] = shifted * waves[1, :, bands] + applied[:, half:]
    copies = [pltpu.make_async_copy(staged, residual.at[:, :, pl.ds(q * half, half)], sems.at[0])]
    if q == 1:
        copies.append(pltpu.make_async_copy(levels, estimate, sems.at[1]))
    for copy in copies:
        copy.start()
    for copy in copies:
        copy.wait()


def swap(x, axis, size, mask):
    return lax.ppermute(x, axis, [(i, i ^ mask) for i in range(size)])


def tree(parts):
    while len(parts) > 1:
        parts = [a + b for a, b in zip(parts[::2], parts[1::2])]
    return parts[0]


def on_device(ga, band, waves, miller, positions, form_factors, coupling, species, block_sizes, occupation):
    _, planes, bands = waves.shape
    half = bands // 2
    nspec, kmax, _ = form_factors.shape
    atoms = species.shape[0]
    rows = PROJ // 4
    depth = depth_of(kmax, nspec)
    positions = positions.T
    form = form_factors.transpose(1, 0, 2)
    coupling = coupling.transpose(1, 0, 2)
    species = species.reshape(1, -1)
    sizes = block_sizes.reshape(1, -1)
    bits = ga.bit_length() - 1
    order = (0, 1)
    params = pltpu.CompilerParams(vmem_limit_bytes=32 * 1024 * 1024)
    hbm = pl.BlockSpec(memory_space=pltpu.HBM)
    vmem = pl.BlockSpec(memory_space=pltpu.VMEM)
    shape = jax.ShapeDtypeStruct
    plain, summed = shape((rows, bands), F32), shape((rows + 8, bands), F32)
    beta = [((2 * rows, 2 * planes), BF16)] * 2
    rhs = [((2 * planes, bands), BF16)] * 2
    tables = [((2 * atoms, planes), BF16)] * 2 + [((2 * depth, planes), BF16), ((PROJ, 2 * depth), BF16), ((PROJ, 2 * atoms), BF16)]
    far_first, across_first, *passed = pl.pallas_call(
        functools.partial(project_send, order),
        name="project_send",
        in_specs=[hbm] * 6,
        out_shape=[plain] * 2 + [shape(*x) for x in beta + rhs + tables],
        scratch_shapes=[
            pltpu.VMEM((2, planes, half), F32),
            pltpu.VMEM(miller.shape, jnp.int32),
            pltpu.VMEM(positions.shape, F32),
            pltpu.VMEM(form.shape, F32),
            pltpu.VMEM((1, atoms), jnp.int32),
            pltpu.VMEM((1, atoms), jnp.int32),
            pltpu.VMEM((depth, planes), F32),
            pltpu.VMEM((2 * rows, bands), F32),
            pltpu.SemaphoreType.DMA((6,)),
        ],
        compiler_params=params,
    )(*(pltpu.with_memory_space_constraint(x, pltpu.HBM) for x in (waves, miller, positions, form, species, sizes)))
    keep_first, near_first, far_second, across_second, keep_second, near_second = pl.pallas_call(
        functools.partial(project_rest, order),
        name="project_rest",
        out_shape=[plain] * 2 + [summed] * 4,
        scratch_shapes=[pltpu.VMEM(*x) for x in beta + rhs] + [pltpu.VMEM((2 * rows, bands), F32)],
        compiler_params=params,
    )(waves, miller, *passed)
    tables = pl.pallas_call(
        apply_tables_kernel,
        name="apply_tables",
        out_shape=[shape((planes, 2 * PROJ), BF16)] * 2 + [shape((PROJ, PROJ), BF16)] * 2,
        scratch_shapes=[pltpu.VMEM((depth, planes), F32), pltpu.VMEM((depth, LANES), F32)],
        compiler_params=params,
    )(miller, positions, form, coupling, species, sizes)
    far_bit, near_bit = 1 << order[0], 1 << order[1]
    masks = {"n": near_bit, "f": far_bit, "a": far_bit | near_bit}
    streams = ((keep_first, near_first, far_first, across_first), (keep_second, near_second, far_second, across_second))
    mine, own, gathered = {}, {}, {}
    for q, (keep, *sent) in enumerate(streams):
        got = [swap(x, "ga", ga, masks[kind]) for kind, x in zip(masks, sent)]
        mine[q] = tree([keep] + got)
    for b in range(2, bits):
        for q in range(2):
            mine[q] = mine[q] + swap(mine[q], "ga", ga, 1 << b)
    for q in range(2):
        own[q] = mine[q][:rows]
        gathered[q] = [swap(own[q], "ga", ga, mask) for mask in masks.values()]
    sums = mine[1][rows:]
    occ = occupation.reshape(2, half)
    residual, levels, share = [], [], []
    for q in range(2):
        rhs_hi, rhs_lo, level, total = pl.pallas_call(
            functools.partial(stats_kernel, order, q),
            out_shape=[shape((2 * PROJ, bands), BF16)] * 2 + [shape((1, half), F32)] * 2,
            scratch_shapes=[pltpu.VMEM((PROJ, bands), F32)],
            compiler_params=params,
        )(own[q], *gathered[q], sums, occ[q : q + 1], tables[2], tables[3], *share)
        share = [total]
        if q == 1:
            energy = tree([total] + [swap(total, "band", band, d) for d in range(1, band)])[0, 0]
        operands = [rhs_hi, rhs_lo, waves, miller, tables[0], tables[1], level, *levels, *residual]
        levels.append(level)
        residual = pl.pallas_call(
            functools.partial(apply_kernel, q),
            in_specs=[vmem] * (7 + q) + [hbm] * q,
            out_specs=[hbm] * (1 + q),
            out_shape=[shape(waves.shape, F32)] + [shape((2, half), F32)] * q,
            scratch_shapes=[pltpu.VMEM((2, planes, half), F32)]
            + [pltpu.VMEM((2, half), F32)] * q
            + [pltpu.SemaphoreType.DMA((2,))],
            input_output_aliases={8: 0} if q else {},
            compiler_params=params,
        )(*operands)
    return residual[0], residual[1].reshape(bands), energy


def solution(mesh):
    in_specs = (
        P(None, "ga", "band"),
        P(None, "ga"),
        P(),
        P(None, None, "ga"),
        P(),
        P(),
        P(),
        P("band"),
    )
    out_specs = (P(None, "ga", "band"), P("band"), P())

    def body(*args):
        return on_device(mesh.shape["ga"], mesh.shape["band"], *args)

    return jax.shard_map(body, mesh=mesh, in_specs=in_specs, out_specs=out_specs, check_vma=False)
```

```python
import functools
import math

import jax
import jax.numpy as jnp
from jax import lax
from jax.experimental import pallas as pl
from jax.experimental.pallas import tpu as pltpu
from jax.sharding import PartitionSpec as P

PROJ = 512
KINETIC_SCALE = 0.005
EPSILON = 1e-06
LANES = 128
CHUNKS = 4
F32 = jnp.float32
BF16 = jnp.bfloat16


def iota(shape, dim):
    return lax.broadcasted_iota(jnp.int32, shape, dim)


def split(x):
    hi = x.astype(BF16)
    return hi, (x - hi.astype(F32)).astype(BF16)


def dot(a, b, contract=((1,), (0,))):
    return lax.dot_general(a, b, (contract, ((), ())), preferred_element_type=F32)


def pick(mask, values, axis):
    return jnp.sum(jnp.where(mask, values, 0.0), axis=axis, keepdims=True)


def depth_of(kmax, nspec):
    return -(-kmax * nspec // 16) * 16


def columns_of(sizes, species):
    atoms = sizes.shape[1]
    here, there = iota((atoms, atoms), 0), iota((atoms, atoms), 1)
    start = pick(there < here, sizes, 1)
    size = pick(there == here, sizes, 1)
    spec = pick(there == here, species, 1)
    return start, size, spec


def rows_by_projector(sizes, species, nspec):
    atoms = sizes.shape[1]
    _, size, spec = columns_of(sizes, species)
    atom = lax.rem(iota((atoms, 2 * atoms), 1), atoms)
    here = iota((atoms, 2 * atoms), 0)
    start = pick(here < atom, size, 0)
    end = start + pick(here == atom, size, 0)
    spec = pick(here == atom, spec, 0)
    place = iota((PROJ, 2 * atoms), 0).astype(F32)
    hot = (place >= start) & (place < end)
    lane = iota((PROJ, 2 * atoms), 1)
    first = hot & (lane < atoms)
    row = pick(first, spec - nspec * start, 1) + nspec * iota((PROJ, 1), 0).astype(F32)
    owner = pick(first, lane.astype(F32), 1)
    return row, jnp.where(hot, 1.0, 0.0).astype(BF16), owner


def rows_by_lane(sizes, species, nspec):
    atoms = sizes.shape[1]
    start, size, spec = columns_of(sizes, species)
    place = iota((atoms, PROJ), 1).astype(F32)
    hot = (place >= start) & (place < start + size)
    lane = iota((1, PROJ), 1).astype(F32)
    channel = lane - pick(hot, start, 0)
    row = nspec * channel + pick(hot, spec, 0)
    owner = pick(hot, iota((atoms, PROJ), 0).astype(F32), 0)
    ones = jnp.where(hot, 1.0, 0.0)
    return row, jnp.concatenate([ones, ones], axis=0).astype(BF16), owner, channel


def column(rows, n):
    size = rows.shape[1]
    return pick(iota((size, size), 0) == iota((size, size), 1), rows[n : n + 1], 1)


def trig(positions, miller):
    cycles = (
        column(positions, 0) * miller[0:1] + column(positions, 1) * miller[1:2] + column(positions, 2) * miller[2:3]
    )
    half = (cycles - jnp.round(cycles)) * math.pi
    sq = half * half
    sine = 1.0 / 6227020800.0
    for n in (39916800.0, 362880.0, 5040.0, 120.0, 6.0, 1.0):
        sine = 1.0 / n - sq * sine
    sine = half * sine
    cosine = 1.0 / 479001600.0
    for n in (3628800.0, 40320.0, 720.0, 24.0, 2.0, 1.0):
        cosine = 1.0 / n - sq * cosine
    return 1.0 - 2.0 * sine * sine, 2.0 * sine * cosine


def stacked(x):
    hi, lo = split(x)
    return jnp.concatenate([hi, lo], axis=0)


def fill_rows(scratch, table):
    kmax, nspec, width = table.shape
    scratch[...] = jnp.zeros(scratch.shape, F32)
    for k in range(kmax):
        scratch[k * nspec : (k + 1) * nspec, 0:width] = table[k]


def hot_rows(row, depth):
    j = lax.rem(iota((PROJ, 2 * depth), 1), depth).astype(F32)
    return jnp.where(row == j, 1.0, 0.0).astype(BF16)


def hot_rows_t(row, depth):
    j = lax.rem(iota((2 * depth, PROJ), 0), depth).astype(F32)
    return jnp.where(row == j, 1.0, 0.0).astype(BF16)


def squares(miller):
    total = miller[0:1] * miller[0:1] + miller[1:2] * miller[1:2] + miller[2:3] * miller[2:3]
    return total


def bit(device, b):
    return lax.rem(lax.shift_right_logical(device, b), 2)


def block_row(device, order, rel, rows):
    index = 2 * lax.bitwise_xor(bit(device, order[0]), rel[0]) + lax.bitwise_xor(bit(device, order[1]), rel[1])
    return pl.multiple_of(index * rows, rows)


def half_row(device, order, rel, rows):
    return pl.multiple_of(lax.bitwise_xor(bit(device, order[0]), rel) * 2 * rows, rows)


def load_bands(re, im, rhs_hi, rhs_lo):
    planes, half = re.shape
    re_hi, re_lo = split(re)
    im_hi, im_lo = split(im)
    for ref, a, b in ((rhs_hi, re_hi, im_hi), (rhs_lo, re_lo, im_lo)):
        ref[0:planes, 0:half] = a
        ref[0:planes, half:] = b
        ref[planes:, 0:half] = b
        ref[planes:, half:] = -a


def band_sums(re, im, miller):
    planes, half = re.shape
    weight = jnp.where(iota((8, planes), 0) == 0, squares(miller), 1.0).astype(BF16)
    scale = jnp.where(iota((8, half), 0) == 0, 0.5 * KINETIC_SCALE, 1.0)
    hi, lo = split(re * re + im * im)
    return scale * (dot(weight, hi) + dot(weight, lo))


def beta_rows(at, count, picks, owners, cosine, sine, radial, hi_ref, lo_ref):
    planes = cosine.shape[1]
    step = count // 2
    for r in range(2):
        source = pl.ds(pl.multiple_of(at + r * step, step), step)
        part = slice(r * step, (r + 1) * step)
        owner = owners[source]
        size = dot(picks[source], radial[...])
        hi, lo = split(size * dot(owner, cosine[...]))
        hi_ref[part, 0:planes] = hi
        lo_ref[part, 0:planes] = lo
        hi, lo = split(-(size * dot(owner, sine[...])))
        hi_ref[part, planes : 2 * planes] = hi
        lo_ref[part, planes : 2 * planes] = lo


def project(hi_ref, lo_ref, rhs_hi, rhs_lo):
    return dot(hi_ref[...], rhs_hi[...]) + dot(hi_ref[...], rhs_lo[...]) + dot(lo_ref[...], rhs_hi[...])


def ordered(device, order, full, outs):
    rows = full.shape[0] // 2
    for second, out in enumerate(outs):
        at = pl.multiple_of(lax.bitwise_xor(bit(device, order[1]), second) * rows, rows)
        out[0:rows] = full[pl.ds(at, rows)]


def project_send(order, waves_in, miller_in, positions_in, form_in, species_in, sizes_in, *refs):
    outs, (hi_ref, lo_ref, rhs_hi, rhs_lo, cosine, sine, radial, picks, owners) = refs[:2], refs[2:11]
    waves, miller, positions, form, species, sizes, table, full, sems = refs[11:]
    half = waves.shape[2]
    pairs = (
        (sizes_in, sizes),
        (species_in, species),
        (miller_in, miller),
        (positions_in, positions),
        (form_in, form),
        (waves_in.at[:, :, pl.ds(0, half)], waves),
    )
    copies = [pltpu.make_async_copy(a, b, sems.at[n]) for n, (a, b) in enumerate(pairs)]
    for copy in copies:
        copy.start()
    device = lax.axis_index("ga")
    for copy in copies[:4]:
        copy.wait()
    cos, sin = trig(positions[...], miller[...].astype(F32))
    cosine[...] = stacked(cos)
    sine[...] = stacked(sin)
    row, owner, _ = rows_by_projector(sizes[...].astype(F32), species[...].astype(F32), form.shape[1])
    picks[...] = hot_rows(row, table.shape[0])
    owners[...] = owner
    copies[4].wait()
    fill_rows(table, form)
    radial[...] = stacked(table[...])
    rows = PROJ // 4
    beta_rows(half_row(device, order, 1, rows), 2 * rows, picks, owners, cosine, sine, radial, hi_ref, lo_ref)
    copies[5].wait()
    load_bands(waves[0], waves[1], rhs_hi, rhs_lo)
    full[...] = project(hi_ref, lo_ref, rhs_hi, rhs_lo)
    ordered(device, order, full, outs)


def project_keep(order, rhs_hi, rhs_lo, cosine, sine, radial, picks, owners, *refs):
    first, (hi_keep, lo_keep, full) = refs[:2], refs[2:]
    rows = PROJ // 4
    device = lax.axis_index("ga")
    beta_rows(half_row(device, order, 0, rows), 2 * rows, picks, owners, cosine, sine, radial, hi_keep, lo_keep)
    full[...] = project(hi_keep, lo_keep, rhs_hi, rhs_lo)
    ordered(device, order, full, first)


def project_second(order, waves, miller, hi_ref, lo_ref, hi_keep, lo_keep, *refs):
    second_send, second_keep, (rhs_hi, rhs_lo, full) = refs[:2], refs[2:4], refs[4:]
    half = waves.shape[2] // 2
    rows = PROJ // 4
    device = lax.axis_index("ga")
    load_bands(waves[0, :, half:], waves[1, :, half:], rhs_hi, rhs_lo)
    m = miller[...].astype(F32)
    sums = [band_sums(waves[0, :, part], waves[1, :, part], m) for part in (slice(0, half), slice(half, 2 * half))]
    tail = jnp.concatenate(sums, axis=1)
    for hi, lo, outs in ((hi_ref, lo_ref, second_send), (hi_keep, lo_keep, second_keep)):
        full[...] = project(hi, lo, rhs_hi, rhs_lo)
        ordered(device, order, full, outs)
        for out in outs:
            out[rows:] = tail


def apply_tables_kernel(miller, positions, form, coupling, species, sizes, hi_ref, lo_ref, dense_hi, dense_lo, table, ctable):
    planes = miller.shape[1]
    nspec = form.shape[1]
    fill_rows(table, form)
    fill_rows(ctable, coupling)
    depth = table.shape[0]
    m = miller[...].astype(F32)
    cosine, sine = trig(positions[...], m)
    cosine, sine = stacked(cosine), stacked(sine)
    radial = stacked(table[...])
    lengths, kinds = sizes[...].astype(F32), species[...].astype(F32)
    row, owners, owner_row, channel = rows_by_lane(lengths, kinds, nspec)
    picks = hot_rows_t(row, depth)
    step = planes // 4
    over = ((0,), (0,))
    for r in range(4):
        part = slice(r * step, (r + 1) * step)
        size = dot(radial[:, part], picks, over)
        hi, lo = split(size * dot(cosine[:, part], owners, over))
        hi_ref[part, 0:PROJ] = hi
        lo_ref[part, 0:PROJ] = lo
        hi, lo = split(-(size * dot(sine[:, part], owners, over)))
        hi_ref[part, PROJ : 2 * PROJ] = hi
        lo_ref[part, PROJ : 2 * PROJ] = lo
    row, _, owner_col = rows_by_projector(lengths, kinds, nspec)
    lines = dot(hot_rows(row, depth), stacked(ctable[...]))
    lines_hi, lines_lo = split(lines)
    spread = jnp.where(iota((ctable.shape[1], PROJ), 0).astype(F32) == channel, 1.0, 0.0).astype(BF16)
    dense = dot(lines_hi, spread) + dot(lines_lo, spread)
    hi, lo = split(jnp.where(owner_col == owner_row, dense, 0.0))
    dense_hi[...] = hi
    dense_lo[...] = lo


def stats_kernel(order, q, own, near, far, across, sums, occupation, dense_hi, dense_lo, *refs):
    rhs_hi, rhs_lo, level_out, share_out, full = refs[-5:]
    rows = PROJ // 4
    half = occupation.shape[1]
    bands = slice(q * half, (q + 1) * half)
    device = lax.axis_index("ga")
    for rel, ref in (((0, 0), own), ((0, 1), near), ((1, 0), far), ((1, 1), across)):
        full[pl.ds(block_row(device, order, rel, rows), rows)] = ref[0:rows]
    proj = full[...]
    p_hi, p_lo = split(proj)
    mixed = dot(dense_hi[...], p_hi) + dot(dense_hi[...], p_lo) + dot(dense_lo[...], p_hi)
    pairs = jnp.sum(proj * mixed, axis=0, keepdims=True)
    nonlocal_sum = pairs[:, 0:half] + pairs[:, half:]
    kin, norm = sums[0:1, bands], sums[1:2, bands]
    level_out[...] = (kin + nonlocal_sum) / (norm + EPSILON)
    share = jnp.sum(occupation[...] * (nonlocal_sum / (norm + EPSILON)), axis=1, keepdims=True)
    share = jnp.broadcast_to(share, share_out.shape)
    for other in refs[:-5]:
        share = other[...] + share
    share_out[...] = share
    m_hi, m_lo = split(mixed)
    for ref, m in ((rhs_hi, m_hi), (rhs_lo, m_lo)):
        ref[0:PROJ] = m
        ref[PROJ:, 0:half] = -m[:, half:]
        ref[PROJ:, half:] = m[:, 0:half]


def apply_kernel(q, rhs_hi, rhs_lo, waves, miller, hi_ref, lo_ref, level, *refs):
    planes = miller.shape[1]
    half = level.shape[1]
    bands = slice(q * half, (q + 1) * half)
    unit = jnp.where(iota((8, half), 0) == 0, 1.0, 0.0).astype(BF16)
    line = jnp.broadcast_to(squares(miller[...].astype(F32)), (8, planes)).astype(BF16)
    shifted = (0.5 * KINETIC_SCALE) * dot(line, unit, ((0,), (0,))) - level[...]
    copies = []
    if q == 0:
        residual, staged, sems = refs
    else:
        before, _, residual, estimate, staged, levels, sems = refs
        levels[0:1] = before[...]
        levels[1:2] = level[...]
        copies.append(pltpu.make_async_copy(levels, estimate, sems.at[2 * CHUNKS]))
        copies[-1].start()
    step = planes // CHUNKS
    for r in range(CHUNKS):
        part = slice(r * step, (r + 1) * step)
        applied = dot(hi_ref[part], rhs_hi[...]) + dot(hi_ref[part], rhs_lo[...]) + dot(lo_ref[part], rhs_hi[...])
        for n in range(2):
            staged[n, r] = shifted[part] * waves[n, part, bands] + applied[:, n * half : (n + 1) * half]
            target = residual.at[n, pl.ds(r * step, step), pl.ds(q * half, half)]
            copies.append(pltpu.make_async_copy(staged.at[n, r], target, sems.at[2 * r + n]))
            copies[-1].start()
    for copy in copies:
        copy.wait()


def swap(x, axis, size, mask):
    return lax.ppermute(x, axis, [(i, i ^ mask) for i in range(size)])


def tree(parts):
    while len(parts) > 1:
        parts = [a + b for a, b in zip(parts[::2], parts[1::2])]
    return parts[0]


def on_device(ga, band, waves, miller, positions, form_factors, coupling, species, block_sizes, occupation):
    _, planes, bands = waves.shape
    half = bands // 2
    nspec, kmax, _ = form_factors.shape
    atoms = species.shape[0]
    rows = PROJ // 4
    depth = depth_of(kmax, nspec)
    positions = positions.T
    form = form_factors.transpose(1, 0, 2)
    coupling = coupling.transpose(1, 0, 2)
    species = species.reshape(1, -1)
    sizes = block_sizes.reshape(1, -1)
    bits = ga.bit_length() - 1
    order = (0, 1)
    params = pltpu.CompilerParams(vmem_limit_bytes=32 * 1024 * 1024)
    hbm = pl.BlockSpec(memory_space=pltpu.HBM)
    vmem = pl.BlockSpec(memory_space=pltpu.VMEM)
    shape = jax.ShapeDtypeStruct
    plain, summed = shape((rows, bands), F32), shape((rows + 8, bands), F32)
    beta = [((2 * rows, 2 * planes), BF16)] * 2
    rhs = [((2 * planes, bands), BF16)] * 2
    tables = [((2 * atoms, planes), BF16)] * 2 + [((2 * depth, planes), BF16), ((PROJ, 2 * depth), BF16), ((PROJ, 2 * atoms), BF16)]
    far_first, across_first, *passed = pl.pallas_call(
        functools.partial(project_send, order),
        name="project_send",
        in_specs=[hbm] * 6,
        out_shape=[plain] * 2 + [shape(*x) for x in beta + rhs + tables],
        scratch_shapes=[
            pltpu.VMEM((2, planes, half), F32),
            pltpu.VMEM(miller.shape, jnp.int32),
            pltpu.VMEM(positions.shape, F32),
            pltpu.VMEM(form.shape, F32),
            pltpu.VMEM((1, atoms), jnp.int32),
            pltpu.VMEM((1, atoms), jnp.int32),
            pltpu.VMEM((depth, planes), F32),
            pltpu.VMEM((2 * rows, bands), F32),
            pltpu.SemaphoreType.DMA((6,)),
        ],
        compiler_params=params,
    )(*(pltpu.with_memory_space_constraint(x, pltpu.HBM) for x in (waves, miller, positions, form, species, sizes)))
    hi_send, lo_send, *halves = passed
    keep_first, near_first, hi_keep, lo_keep = pl.pallas_call(
        functools.partial(project_keep, order),
        name="project_keep",
        out_shape=[plain] * 2 + [shape(*x) for x in beta],
        scratch_shapes=[pltpu.VMEM((2 * rows, bands), F32)],
        compiler_params=params,
    )(*halves)
    far_second, across_second, keep_second, near_second = pl.pallas_call(
        functools.partial(project_second, order),
        name="project_second",
        out_shape=[summed] * 4,
        scratch_shapes=[pltpu.VMEM(*x) for x in rhs] + [pltpu.VMEM((2 * rows, bands), F32)],
        compiler_params=params,
    )(waves, miller, hi_send, lo_send, hi_keep, lo_keep)
    tables = pl.pallas_call(
        apply_tables_kernel,
        name="apply_tables",
        out_shape=[shape((planes, 2 * PROJ), BF16)] * 2 + [shape((PROJ, PROJ), BF16)] * 2,
        scratch_shapes=[pltpu.VMEM((depth, planes), F32), pltpu.VMEM((depth, LANES), F32)],
        compiler_params=params,
    )(miller, positions, form, coupling, species, sizes)
    far_bit, near_bit = 1 << order[0], 1 << order[1]
    masks = {"n": near_bit, "f": far_bit, "a": far_bit | near_bit}
    streams = ((keep_first, near_first, far_first, across_first), (keep_second, near_second, far_second, across_second))
    mine, own, gathered = {}, {}, {}
    for q, (keep, *sent) in enumerate(streams):
        got = [swap(x, "ga", ga, masks[kind]) for kind, x in zip(masks, sent)]
        mine[q] = tree([keep] + got)
    for b in range(2, bits):
        for q in range(2):
            mine[q] = mine[q] + swap(mine[q], "ga", ga, 1 << b)
    for q in range(2):
        own[q] = mine[q][:rows]
        gathered[q] = [swap(own[q], "ga", ga, mask) for mask in masks.values()]
    sums = mine[1][rows:]
    occ = occupation.reshape(2, half)
    residual, levels, share = [], [], []
    for q in range(2):
        rhs_hi, rhs_lo, level, total = pl.pallas_call(
            functools.partial(stats_kernel, order, q),
            out_shape=[shape((2 * PROJ, bands), BF16)] * 2 + [shape((1, half), F32)] * 2,
            scratch_shapes=[pltpu.VMEM((PROJ, bands), F32)],
            compiler_params=params,
        )(own[q], *gathered[q], sums, occ[q : q + 1], tables[2], tables[3], *share)
        share = [total]
        if q == 1:
            energy = tree([total] + [swap(total, "band", band, d) for d in range(1, band)])[0, 0]
        operands = [rhs_hi, rhs_lo, waves, miller, tables[0], tables[1], level, *levels, *residual]
        levels.append(level)
        residual = pl.pallas_call(
            functools.partial(apply_kernel, q),
            in_specs=[vmem] * (7 + q) + [hbm] * q,
            out_specs=[hbm] * (1 + q),
            out_shape=[shape(waves.shape, F32)] + [shape((2, half), F32)] * q,
            scratch_shapes=[pltpu.VMEM((2, CHUNKS, planes // CHUNKS, half), F32)]
            + [pltpu.VMEM((2, half), F32)] * q
            + [pltpu.SemaphoreType.DMA((2 * CHUNKS + 1,))],
            input_output_aliases={8: 0} if q else {},
            compiler_params=params,
        )(*operands)
    return residual[0], residual[1].reshape(bands), energy


def solution(mesh):
    in_specs = (
        P(None, "ga", "band"),
        P(None, "ga"),
        P(),
        P(None, None, "ga"),
        P(),
        P(),
        P(),
        P("band"),
    )
    out_specs = (P(None, "ga", "band"), P("band"), P())

    def body(*args):
        return on_device(mesh.shape["ga"], mesh.shape["band"], *args)

    return jax.shard_map(body, mesh=mesh, in_specs=in_specs, out_specs=out_specs, check_vma=False)
```

```python
import functools
import math

import jax
import jax.numpy as jnp
from jax import lax
from jax.experimental import pallas as pl
from jax.experimental.pallas import tpu as pltpu
from jax.sharding import PartitionSpec as P

PROJ = 512
KINETIC_SCALE = 0.005
EPSILON = 1e-06
LANES = 128
CHUNKS = 4
F32 = jnp.float32
BF16 = jnp.bfloat16


def iota(shape, dim):
    return lax.broadcasted_iota(jnp.int32, shape, dim)


def split(x):
    hi = x.astype(BF16)
    return hi, (x - hi.astype(F32)).astype(BF16)


def dot(a, b, contract=((1,), (0,))):
    return lax.dot_general(a, b, (contract, ((), ())), preferred_element_type=F32)


def pick(mask, values, axis):
    return jnp.sum(jnp.where(mask, values, 0.0), axis=axis, keepdims=True)


def depth_of(kmax, nspec):
    return -(-kmax * nspec // 16) * 16


def columns_of(sizes, species):
    atoms = sizes.shape[1]
    here, there = iota((atoms, atoms), 0), iota((atoms, atoms), 1)
    start = pick(there < here, sizes, 1)
    size = pick(there == here, sizes, 1)
    spec = pick(there == here, species, 1)
    return start, size, spec


def rows_by_projector(sizes, species, nspec):
    atoms = sizes.shape[1]
    _, size, spec = columns_of(sizes, species)
    atom = lax.rem(iota((atoms, 2 * atoms), 1), atoms)
    here = iota((atoms, 2 * atoms), 0)
    start = pick(here < atom, size, 0)
    end = start + pick(here == atom, size, 0)
    spec = pick(here == atom, spec, 0)
    place = iota((PROJ, 2 * atoms), 0).astype(F32)
    hot = (place >= start) & (place < end)
    lane = iota((PROJ, 2 * atoms), 1)
    first = hot & (lane < atoms)
    row = pick(first, spec - nspec * start, 1) + nspec * iota((PROJ, 1), 0).astype(F32)
    owner = pick(first, lane.astype(F32), 1)
    return row, jnp.where(hot, 1.0, 0.0).astype(BF16), owner


def rows_by_lane(sizes, species, nspec):
    atoms = sizes.shape[1]
    start, size, spec = columns_of(sizes, species)
    place = iota((atoms, PROJ), 1).astype(F32)
    hot = (place >= start) & (place < start + size)
    lane = iota((1, PROJ), 1).astype(F32)
    channel = lane - pick(hot, start, 0)
    row = nspec * channel + pick(hot, spec, 0)
    owner = pick(hot, iota((atoms, PROJ), 0).astype(F32), 0)
    ones = jnp.where(hot, 1.0, 0.0)
    return row, jnp.concatenate([ones, ones], axis=0).astype(BF16), owner, channel


def column(rows, n):
    size = rows.shape[1]
    return pick(iota((size, size), 0) == iota((size, size), 1), rows[n : n + 1], 1)


def trig(positions, miller):
    cycles = (
        column(positions, 0) * miller[0:1] + column(positions, 1) * miller[1:2] + column(positions, 2) * miller[2:3]
    )
    half = (cycles - jnp.round(cycles)) * math.pi
    sq = half * half
    sine = 1.0 / 6227020800.0
    for n in (39916800.0, 362880.0, 5040.0, 120.0, 6.0, 1.0):
        sine = 1.0 / n - sq * sine
    sine = half * sine
    cosine = 1.0 / 479001600.0
    for n in (3628800.0, 40320.0, 720.0, 24.0, 2.0, 1.0):
        cosine = 1.0 / n - sq * cosine
    return 1.0 - 2.0 * sine * sine, 2.0 * sine * cosine


def stacked(x):
    hi, lo = split(x)
    return jnp.concatenate([hi, lo], axis=0)


def fill_rows(scratch, table):
    kmax, nspec, width = table.shape
    scratch[...] = jnp.zeros(scratch.shape, F32)
    for k in range(kmax):
        scratch[k * nspec : (k + 1) * nspec, 0:width] = table[k]


def hot_rows(row, depth):
    j = lax.rem(iota((PROJ, 2 * depth), 1), depth).astype(F32)
    return jnp.where(row == j, 1.0, 0.0).astype(BF16)


def hot_rows_t(row, depth):
    j = lax.rem(iota((2 * depth, PROJ), 0), depth).astype(F32)
    return jnp.where(row == j, 1.0, 0.0).astype(BF16)


def squares(miller):
    total = miller[0:1] * miller[0:1] + miller[1:2] * miller[1:2] + miller[2:3] * miller[2:3]
    return total


def bit(device, b):
    return lax.rem(lax.shift_right_logical(device, b), 2)


def block_row(device, order, rel, rows):
    index = 2 * lax.bitwise_xor(bit(device, order[0]), rel[0]) + lax.bitwise_xor(bit(device, order[1]), rel[1])
    return pl.multiple_of(index * rows, rows)


def half_row(device, order, rel, rows):
    return pl.multiple_of(lax.bitwise_xor(bit(device, order[0]), rel) * 2 * rows, rows)


def load_bands(re, im, rhs_hi, rhs_lo):
    planes, half = re.shape
    re_hi, re_lo = split(re)
    im_hi, im_lo = split(im)
    for ref, a, b in ((rhs_hi, re_hi, im_hi), (rhs_lo, re_lo, im_lo)):
        ref[0:planes, 0:half] = a
        ref[0:planes, half:] = b
        ref[planes:, 0:half] = b
        ref[planes:, half:] = -a


def band_sums(re, im, miller):
    planes, half = re.shape
    weight = jnp.where(iota((8, planes), 0) == 0, squares(miller), 1.0).astype(BF16)
    scale = jnp.where(iota((8, half), 0) == 0, 0.5 * KINETIC_SCALE, 1.0)
    hi, lo = split(re * re + im * im)
    return scale * (dot(weight, hi) + dot(weight, lo))


def beta_rows(at, count, picks, owners, cosine, sine, radial, hi_ref, lo_ref):
    planes = cosine.shape[1]
    step = count // 2
    for r in range(2):
        source = pl.ds(pl.multiple_of(at + r * step, step), step)
        part = slice(r * step, (r + 1) * step)
        owner = owners[source]
        size = dot(picks[source], radial[...])
        hi, lo = split(size * dot(owner, cosine[...]))
        hi_ref[part, 0:planes] = hi
        lo_ref[part, 0:planes] = lo
        hi, lo = split(-(size * dot(owner, sine[...])))
        hi_ref[part, planes : 2 * planes] = hi
        lo_ref[part, planes : 2 * planes] = lo


def project(hi_ref, lo_ref, rhs_hi, rhs_lo):
    return dot(hi_ref[...], rhs_hi[...]) + dot(hi_ref[...], rhs_lo[...]) + dot(lo_ref[...], rhs_hi[...])


def ordered(device, order, full, outs):
    rows = full.shape[0] // 2
    for second, out in enumerate(outs):
        at = pl.multiple_of(lax.bitwise_xor(bit(device, order[1]), second) * rows, rows)
        out[0:rows] = full[pl.ds(at, rows)]


def project_send(order, waves_in, miller_in, positions_in, form_in, species_in, sizes_in, *refs):
    outs, (hi_ref, lo_ref, rhs_hi, rhs_lo, cosine, sine, radial, picks, owners) = refs[:2], refs[2:11]
    waves, miller, positions, form, species, sizes, table, full, sems = refs[11:]
    half = waves.shape[2]
    pairs = (
        (sizes_in, sizes),
        (species_in, species),
        (miller_in, miller),
        (positions_in, positions),
        (form_in, form),
        (waves_in.at[:, :, pl.ds(0, half)], waves),
    )
    copies = [pltpu.make_async_copy(a, b, sems.at[n]) for n, (a, b) in enumerate(pairs)]
    for copy in copies:
        copy.start()
    device = lax.axis_index("ga")
    for copy in copies[:4]:
        copy.wait()
    cos, sin = trig(positions[...], miller[...].astype(F32))
    cosine[...] = stacked(cos)
    sine[...] = stacked(sin)
    row, owner, _ = rows_by_projector(sizes[...].astype(F32), species[...].astype(F32), form.shape[1])
    picks[...] = hot_rows(row, table.shape[0])
    owners[...] = owner
    copies[4].wait()
    fill_rows(table, form)
    radial[...] = stacked(table[...])
    rows = PROJ // 4
    beta_rows(half_row(device, order, 1, rows), 2 * rows, picks, owners, cosine, sine, radial, hi_ref, lo_ref)
    copies[5].wait()
    load_bands(waves[0], waves[1], rhs_hi, rhs_lo)
    full[...] = project(hi_ref, lo_ref, rhs_hi, rhs_lo)
    ordered(device, order, full, outs)


def project_keep(order, rhs_hi, rhs_lo, cosine, sine, radial, picks, owners, *refs):
    first, (hi_keep, lo_keep, full) = refs[:2], refs[2:]
    rows = PROJ // 4
    device = lax.axis_index("ga")
    beta_rows(half_row(device, order, 0, rows), 2 * rows, picks, owners, cosine, sine, radial, hi_keep, lo_keep)
    full[...] = project(hi_keep, lo_keep, rhs_hi, rhs_lo)
    ordered(device, order, full, first)


def project_second(order, waves, miller, hi_ref, lo_ref, hi_keep, lo_keep, *refs):
    second_send, second_keep, (rhs_hi, rhs_lo, full) = refs[:2], refs[2:4], refs[4:]
    half = waves.shape[2] // 2
    rows = PROJ // 4
    device = lax.axis_index("ga")
    load_bands(waves[0, :, half:], waves[1, :, half:], rhs_hi, rhs_lo)
    m = miller[...].astype(F32)
    sums = [band_sums(waves[0, :, part], waves[1, :, part], m) for part in (slice(0, half), slice(half, 2 * half))]
    tail = jnp.concatenate(sums, axis=1)
    for hi, lo, outs in ((hi_ref, lo_ref, second_send), (hi_keep, lo_keep, second_keep)):
        full[...] = project(hi, lo, rhs_hi, rhs_lo)
        ordered(device, order, full, outs)
        for out in outs:
            out[rows:] = tail


def apply_tables_kernel(miller, positions, form, coupling, species, sizes, hi_ref, lo_ref, dense_hi, dense_lo, kinetic, table, ctable):
    planes = miller.shape[1]
    nspec = form.shape[1]
    fill_rows(table, form)
    fill_rows(ctable, coupling)
    depth = table.shape[0]
    m = miller[...].astype(F32)
    cosine, sine = trig(positions[...], m)
    cosine, sine = stacked(cosine), stacked(sine)
    radial = stacked(table[...])
    lengths, kinds = sizes[...].astype(F32), species[...].astype(F32)
    row, owners, owner_row, channel = rows_by_lane(lengths, kinds, nspec)
    picks = hot_rows_t(row, depth)
    step = planes // 4
    over = ((0,), (0,))
    for r in range(4):
        part = slice(r * step, (r + 1) * step)
        size = dot(radial[:, part], picks, over)
        hi, lo = split(size * dot(cosine[:, part], owners, over))
        hi_ref[part, 0:PROJ] = hi
        lo_ref[part, 0:PROJ] = lo
        hi, lo = split(-(size * dot(sine[:, part], owners, over)))
        hi_ref[part, PROJ : 2 * PROJ] = hi
        lo_ref[part, PROJ : 2 * PROJ] = lo
    row, _, owner_col = rows_by_projector(lengths, kinds, nspec)
    lines = dot(hot_rows(row, depth), stacked(ctable[...]))
    lines_hi, lines_lo = split(lines)
    spread = jnp.where(iota((ctable.shape[1], PROJ), 0).astype(F32) == channel, 1.0, 0.0).astype(BF16)
    dense = dot(lines_hi, spread) + dot(lines_lo, spread)
    hi, lo = split(jnp.where(owner_col == owner_row, dense, 0.0))
    dense_hi[...] = hi
    dense_lo[...] = lo
    unit = jnp.where(iota((8, kinetic.shape[1]), 0) == 0, 1.0, 0.0).astype(BF16)
    line = jnp.broadcast_to(squares(m), (8, planes)).astype(BF16)
    kinetic[...] = (0.5 * KINETIC_SCALE) * dot(line, unit, over)


def stats_kernel(order, q, own, near, far, across, sums, occupation, dense_hi, dense_lo, *refs):
    rhs_hi, rhs_lo, level_out, share_out, full = refs[-5:]
    rows = PROJ // 4
    half = occupation.shape[1]
    bands = slice(q * half, (q + 1) * half)
    device = lax.axis_index("ga")
    for rel, ref in (((0, 0), own), ((0, 1), near), ((1, 0), far), ((1, 1), across)):
        full[pl.ds(block_row(device, order, rel, rows), rows)] = ref[0:rows]
    proj = full[...]
    p_hi, p_lo = split(proj)
    mixed = dot(dense_hi[...], p_hi) + dot(dense_hi[...], p_lo) + dot(dense_lo[...], p_hi)
    pairs = jnp.sum(proj * mixed, axis=0, keepdims=True)
    nonlocal_sum = pairs[:, 0:half] + pairs[:, half:]
    kin, norm = sums[0:1, bands], sums[1:2, bands]
    level_out[...] = (kin + nonlocal_sum) / (norm + EPSILON)
    share = jnp.sum(occupation[...] * (nonlocal_sum / (norm + EPSILON)), axis=1, keepdims=True)
    share = jnp.broadcast_to(share, share_out.shape)
    for other in refs[:-5]:
        share = other[...] + share
    share_out[...] = share
    m_hi, m_lo = split(mixed)
    for ref, m in ((rhs_hi, m_hi), (rhs_lo, m_lo)):
        ref[0:PROJ] = m
        ref[PROJ:, 0:half] = -m[:, half:]
        ref[PROJ:, half:] = m[:, 0:half]


def apply_kernel(q, rhs_hi, rhs_lo, waves, kinetic, hi_ref, lo_ref, level, *refs):
    planes, half = kinetic.shape
    bands = slice(q * half, (q + 1) * half)
    copies = []
    if q == 0:
        residual, staged, sems = refs
    else:
        before, _, residual, estimate, staged, levels, sems = refs
        levels[0:1] = before[...]
        levels[1:2] = level[...]
        copies.append(pltpu.make_async_copy(levels, estimate, sems.at[2 * CHUNKS]))
        copies[-1].start()
    step = planes // CHUNKS
    for r in range(CHUNKS):
        part = slice(r * step, (r + 1) * step)
        applied = dot(hi_ref[part], rhs_hi[...]) + dot(hi_ref[part], rhs_lo[...]) + dot(lo_ref[part], rhs_hi[...])
        for n in range(2):
            staged[n, r] = (kinetic[part] - level[...]) * waves[n, part, bands] + applied[:, n * half : (n + 1) * half]
            target = residual.at[n, pl.ds(r * step, step), pl.ds(q * half, half)]
            copies.append(pltpu.make_async_copy(staged.at[n, r], target, sems.at[2 * r + n]))
            copies[-1].start()
    for copy in copies:
        copy.wait()


def swap(x, axis, size, mask):
    return lax.ppermute(x, axis, [(i, i ^ mask) for i in range(size)])


def tree(parts):
    while len(parts) > 1:
        parts = [a + b for a, b in zip(parts[::2], parts[1::2])]
    return parts[0]


def on_device(ga, band, waves, miller, positions, form_factors, coupling, species, block_sizes, occupation):
    _, planes, bands = waves.shape
    half = bands // 2
    nspec, kmax, _ = form_factors.shape
    atoms = species.shape[0]
    rows = PROJ // 4
    depth = depth_of(kmax, nspec)
    positions = positions.T
    form = form_factors.transpose(1, 0, 2)
    coupling = coupling.transpose(1, 0, 2)
    species = species.reshape(1, -1)
    sizes = block_sizes.reshape(1, -1)
    bits = ga.bit_length() - 1
    order = (0, 1)
    params = pltpu.CompilerParams(vmem_limit_bytes=32 * 1024 * 1024)
    hbm = pl.BlockSpec(memory_space=pltpu.HBM)
    vmem = pl.BlockSpec(memory_space=pltpu.VMEM)
    shape = jax.ShapeDtypeStruct
    plain, summed = shape((rows, bands), F32), shape((rows + 8, bands), F32)
    beta = [((2 * rows, 2 * planes), BF16)] * 2
    rhs = [((2 * planes, bands), BF16)] * 2
    tables = [((2 * atoms, planes), BF16)] * 2 + [((2 * depth, planes), BF16), ((PROJ, 2 * depth), BF16), ((PROJ, 2 * atoms), BF16)]
    far_first, across_first, *passed = pl.pallas_call(
        functools.partial(project_send, order),
        name="project_send",
        in_specs=[hbm] * 6,
        out_shape=[plain] * 2 + [shape(*x) for x in beta + rhs + tables],
        scratch_shapes=[
            pltpu.VMEM((2, planes, half), F32),
            pltpu.VMEM(miller.shape, jnp.int32),
            pltpu.VMEM(positions.shape, F32),
            pltpu.VMEM(form.shape, F32),
            pltpu.VMEM((1, atoms), jnp.int32),
            pltpu.VMEM((1, atoms), jnp.int32),
            pltpu.VMEM((depth, planes), F32),
            pltpu.VMEM((2 * rows, bands), F32),
            pltpu.SemaphoreType.DMA((6,)),
        ],
        compiler_params=params,
    )(*(pltpu.with_memory_space_constraint(x, pltpu.HBM) for x in (waves, miller, positions, form, species, sizes)))
    hi_send, lo_send, *halves = passed
    keep_first, near_first, hi_keep, lo_keep = pl.pallas_call(
        functools.partial(project_keep, order),
        name="project_keep",
        out_shape=[plain] * 2 + [shape(*x) for x in beta],
        scratch_shapes=[pltpu.VMEM((2 * rows, bands), F32)],
        compiler_params=params,
    )(*halves)
    far_second, across_second, keep_second, near_second = pl.pallas_call(
        functools.partial(project_second, order),
        name="project_second",
        out_shape=[summed] * 4,
        scratch_shapes=[pltpu.VMEM(*x) for x in rhs] + [pltpu.VMEM((2 * rows, bands), F32)],
        compiler_params=params,
    )(waves, miller, hi_send, lo_send, hi_keep, lo_keep)
    tables = pl.pallas_call(
        apply_tables_kernel,
        name="apply_tables",
        out_shape=[shape((planes, 2 * PROJ), BF16)] * 2 + [shape((PROJ, PROJ), BF16)] * 2 + [shape((planes, half), F32)],
        scratch_shapes=[pltpu.VMEM((depth, planes), F32), pltpu.VMEM((depth, LANES), F32)],
        compiler_params=params,
    )(miller, positions, form, coupling, species, sizes)
    far_bit, near_bit = 1 << order[0], 1 << order[1]
    masks = {"n": near_bit, "f": far_bit, "a": far_bit | near_bit}
    streams = ((keep_first, near_first, far_first, across_first), (keep_second, near_second, far_second, across_second))
    mine, own, gathered = {}, {}, {}
    for q, (keep, *sent) in enumerate(streams):
        got = [swap(x, "ga", ga, masks[kind]) for kind, x in zip(masks, sent)]
        mine[q] = tree([keep] + got)
    for b in range(2, bits):
        for q in range(2):
            mine[q] = mine[q] + swap(mine[q], "ga", ga, 1 << b)
    for q in range(2):
        own[q] = mine[q][:rows]
        gathered[q] = [swap(own[q], "ga", ga, mask) for mask in masks.values()]
    sums = mine[1][rows:]
    occ = occupation.reshape(2, half)
    residual, levels, share = [], [], []
    for q in range(2):
        rhs_hi, rhs_lo, level, total = pl.pallas_call(
            functools.partial(stats_kernel, order, q),
            out_shape=[shape((2 * PROJ, bands), BF16)] * 2 + [shape((1, half), F32)] * 2,
            scratch_shapes=[pltpu.VMEM((PROJ, bands), F32)],
            compiler_params=params,
        )(own[q], *gathered[q], sums, occ[q : q + 1], tables[2], tables[3], *share)
        share = [total]
        if q == 1:
            energy = tree([total] + [swap(total, "band", band, d) for d in range(1, band)])[0, 0]
        operands = [rhs_hi, rhs_lo, waves, tables[4], tables[0], tables[1], level, *levels, *residual]
        levels.append(level)
        residual = pl.pallas_call(
            functools.partial(apply_kernel, q),
            in_specs=[vmem] * (7 + q) + [hbm] * q,
            out_specs=[hbm] * (1 + q),
            out_shape=[shape(waves.shape, F32)] + [shape((2, half), F32)] * q,
            scratch_shapes=[pltpu.VMEM((2, CHUNKS, planes // CHUNKS, half), F32)]
            + [pltpu.VMEM((2, half), F32)] * q
            + [pltpu.SemaphoreType.DMA((2 * CHUNKS + 1,))],
            input_output_aliases={8: 0} if q else {},
            compiler_params=params,
        )(*operands)
    return residual[0], residual[1].reshape(bands), energy


def solution(mesh):
    in_specs = (
        P(None, "ga", "band"),
        P(None, "ga"),
        P(),
        P(None, None, "ga"),
        P(),
        P(),
        P(),
        P("band"),
    )
    out_specs = (P(None, "ga", "band"), P("band"), P())

    def body(*args):
        return on_device(mesh.shape["ga"], mesh.shape["band"], *args)

    return jax.shard_map(body, mesh=mesh, in_specs=in_specs, out_specs=out_specs, check_vma=False)
```
